256 devices in a mesh: rows: 64 (over x, z_hi, y), grp: 4 (over z_lo, core).
Axes of the slice: x: 4, y: 4, z: 8 (z_hi: 4, z_lo: 2; z = z_hi * 2 + z_lo), core: 2. Of those that a mesh axis runs over, the one named last changes fastest.
Arguments:
- vector: float32 [1024, 16, 384], P(('rows', 'grp')), may hold values from -20 to 20
- near_cols: int32 [1024, 3], P(('rows', 'grp')), may hold values from 0 to 1023, as said below
- near_blocks: bfloat16 [1024, 3, 384, 384], P(('rows', 'grp')), may hold values from -2 to 2
- col_basis: bfloat16 [1024, 32, 384], P(('rows', 'grp')), may hold values from -0.3125 to 0.3125
- row_basis: bfloat16 [1024, 32, 384], P(('rows', 'grp')), may hold values from -1 to 1
- leaf_far: int32 [1024, 8], P(('rows', 'grp')), may hold values from 0 to 1023, as said below
- leaf_coupling: bfloat16 [1024, 32, 256], P(('rows', 'grp')), may hold values from -0.375 to 0.375
- leaf_transfer: float32 [1024, 32, 32], P(('rows', 'grp')), may hold values from -0.5 to 0.5
- box_far: int32 [256, 4], P(('rows', 'grp')), may hold values from 0 to 255, as said below
- box_coupling: bfloat16 [256, 32, 128], P(('rows', 'grp')), may hold values from -0.5 to 0.5
- box_transfer: float32 [256, 32, 32], P(('rows', 'grp')), may hold values from -1 to 1
- coarse_far: int32 [64, 4], P('rows'), may hold values from 0 to 63, as said below
- coarse_coupling: bfloat16 [64, 32, 128], P('rows'), may hold values from -0.5 to 0.5
Outputs:
- basis: float32 [1024, 16, 384], P(('rows', 'grp'))
- remainder: float32 [1024, 16, 384], P(('rows', 'grp'))
- hessenberg: float32 [16, 5], replicated
The draws below stay inside these ranges and needn't reach their ends.
Inputs may be any that keep to these rules, and one draw needn't show every extreme that they name: `near_cols`: entry 0 of leaf l is l itself; the other entries are distinct leaves l + o with 0 < |o| <= 4. `leaf_far`: the entries of leaf l are distinct leaves g with |g - l| > 4 and |g // 16 - l // 16| <= 1. `box_far`: the entries of box x are distinct boxes y with |y - x| > 1 and |y // 4 - x // 4| <= 1. `coarse_far`: the entries of group g are distinct groups h with |h - g| > 1.
All inputs are finite; a program needn't handle non-finite values.
Results may differ from the reference program's by a relative error of at most 0.015.
Values may be sent and summed in bfloat16 or wider, within the bound.
No kernel may reach another device: no remote copies, remote signals or barrier semaphores. Data moves between devices by JAX's collectives and lax.ppermute only.
A program may use at most 64 MiB of HBM per device.

```python
import jax
import jax.numpy as jnp
from jax import lax

LP = 128
R = 32
NRHS = 16
LD = 4
KN = 3
KF = 8
KB = 4
KC = 4
BOX_GROUP = 4
GROUPS = 64
BOXES = 256
LEAVES = 1024
GL = 16


def pick_distinct(key, candidates, valid, count):
    total_rows, span = candidates.shape
    offsets = jnp.arange(span, dtype=jnp.int32)[None, :]
    raw_scores = jax.random.randint(key, (total_rows, span), 0, 1 << 16, dtype=jnp.int32)
    scores = jnp.where(valid, raw_scores * span + offsets, -1 - offsets)
    picked_values, picked = lax.top_k(scores, count)
    return jnp.take_along_axis(candidates, picked, axis=1).astype(jnp.int32)


def draw_vector(key, part):
    key_base, key_rough = jax.random.split(jax.random.fold_in(key, 11))
    shape = (LEAVES, NRHS, 3 * LP)
    ramp = jnp.arange(LEAVES, dtype=jnp.float32)[:, None, None] / max(LEAVES - 1, 1)
    rough = jnp.exp(jax.random.uniform(key_rough, (LEAVES, NRHS, 1), jnp.float32, -0.35, 0.35))
    base = jax.random.truncated_normal(key_base, -4.0, 4.0, shape, jnp.float32)
    scale = 1.0 + 2.0 * ramp
    return (base * scale * rough).astype(jnp.float32)


def draw_near_blocks(key, part):
    base_key = jax.random.fold_in(key, 61)
    width = 3 * LP

    def one_leaf(leaf):
        key_self, key_rest = jax.random.split(jax.random.fold_in(base_key, leaf))
        raw_self = jax.random.truncated_normal(key_self, -4.0, 4.0, (width, width), jnp.float32)
        raw_rest = jax.random.truncated_normal(key_rest, -4.0, 4.0, (KN - 1, width, width), jnp.float32)
        own_block = (raw_self + raw_self.T) * (1.5 / (2.0 * width) ** 0.5)
        other_blocks = raw_rest / (width * KN) ** 0.5
        return jnp.concatenate([own_block[None], other_blocks], axis=0).astype(jnp.bfloat16)
    return lax.map(one_leaf, jnp.arange(LEAVES, dtype=jnp.int32))


def draw_near_cols(key, part):
    leaf = jnp.arange(LEAVES, dtype=jnp.int32)[:, None]
    offsets = jnp.concatenate([jnp.arange(-LD, 0, dtype=jnp.int32), jnp.arange(1, LD + 1, dtype=jnp.int32)])[None, :]
    candidates = leaf + offsets
    valid = (candidates >= 0) & (candidates < LEAVES)
    others = pick_distinct(jax.random.fold_in(key, 21), candidates, valid, KN - 1)
    return jnp.concatenate([leaf, others], axis=1).astype(jnp.int32)


def draw_leaf_far(key, part):
    leaf = jnp.arange(LEAVES, dtype=jnp.int32)[:, None]
    slots = jnp.arange(3 * GL, dtype=jnp.int32)[None, :]
    candidates = (leaf // GL - 1) * GL + slots
    valid = (candidates >= 0) & (candidates < LEAVES) & (jnp.abs(candidates - leaf) > LD)
    return pick_distinct(jax.random.fold_in(key, 31), candidates, valid, KF)


def draw_box_far(key, part):
    box_index = jnp.arange(BOXES, dtype=jnp.int32)[:, None]
    slots = jnp.arange(3 * BOX_GROUP, dtype=jnp.int32)[None, :]
    candidates = (box_index // BOX_GROUP - 1) * BOX_GROUP + slots
    valid = (candidates >= 0) & (candidates < BOXES) & (jnp.abs(candidates - box_index) > 1)
    return pick_distinct(jax.random.fold_in(key, 41), candidates, valid, KB)


def draw_coarse_far(key, part):
    group_index = jnp.arange(GROUPS, dtype=jnp.int32)[:, None]
    candidates = jnp.broadcast_to(jnp.arange(GROUPS, dtype=jnp.int32)[None, :], (GROUPS, GROUPS))
    valid = jnp.abs(candidates - group_index) > 1
    return pick_distinct(jax.random.fold_in(key, 51), candidates, valid, KC)


def block_levels(stream_key, shape, cuts, least, top_value):
    gain = 1.0
    for dim, parts in cuts:
        steps = jax.random.uniform(jax.random.fold_in(jax.random.fold_in(stream_key, 6), dim), (parts,), jnp.float32, least / len(cuts), top_value / len(cuts))
        gain = gain * jnp.repeat(jnp.exp(steps), shape[dim] // parts).reshape((-1,) + (1,) * (len(shape) - 1 - dim))
    return gain


def noise(own_key, extent, scale, bound, cuts=(), kind=jnp.bfloat16):
    entries = scale * jax.random.normal(own_key, extent, jnp.float32)
    if cuts:
        entries = entries * block_levels(own_key, extent, cuts, -0.22, 0.18)
    return jnp.clip(entries, -bound, bound).astype(kind)


def setup_inputs(seed: int = 0) -> dict:
    arg_keys = jax.random.split(jax.random.key(seed), 14)
    vector = draw_vector(jax.random.fold_in(arg_keys[13], 71), 0)
    near_cols = draw_near_cols(jax.random.fold_in(arg_keys[13], 71), 0)
    near_blocks = draw_near_blocks(jax.random.fold_in(arg_keys[13], 71), 0)
    col_basis = noise(arg_keys[3], (LEAVES, R, 3 * LP), (3 * LP) ** -0.5, 0.3125, ((0, 256),))
    row_basis = noise(arg_keys[4], (LEAVES, R, 3 * LP), R ** -0.5, 1.0, ((0, 256),))
    leaf_far = draw_leaf_far(jax.random.fold_in(arg_keys[13], 71), 0)
    leaf_coupling = noise(arg_keys[6], (LEAVES, R, KF * R), (KF * R) ** -0.5, 0.375, ((0, 256),))
    leaf_transfer = noise(arg_keys[7], (LEAVES, R, R), (LD * R) ** -0.5, 0.5, ((0, 256),), jnp.float32)
    box_far = draw_box_far(jax.random.fold_in(arg_keys[13], 71), 0)
    box_coupling = noise(arg_keys[9], (BOXES, R, KB * R), (KB * R) ** -0.5, 0.5, ((0, 256),))
    box_transfer = noise(arg_keys[10], (BOXES, R, R), R ** -0.5, 1.0, ((0, 256),), jnp.float32)
    coarse_far = draw_coarse_far(jax.random.fold_in(arg_keys[13], 71), 0)
    coarse_coupling = noise(arg_keys[12], (GROUPS, R, KC * R), (KC * R) ** -0.5, 0.5, ((0, 64),))
    return {"vector": vector, "near_cols": near_cols, "near_blocks": near_blocks, "col_basis": col_basis, "row_basis": row_basis, "leaf_far": leaf_far, "leaf_coupling": leaf_coupling, "leaf_transfer": leaf_transfer, "box_far": box_far, "box_coupling": box_coupling, "box_transfer": box_transfer, "coarse_far": coarse_far, "coarse_coupling": coarse_coupling}


highest = lax.Precision.HIGHEST
epsilon = 1e-06

def to_float(array):
    return array.astype(jnp.float32)

def near_term(field_bf, near_cols, near_blocks):
    columns = near_cols.reshape(BOXES, LD, KN)
    blocks = near_blocks.reshape(BOXES, LD, KN, 3 * LP, 3 * LP)

    def per_box(operands):
        picked = to_float(jnp.take(field_bf, operands[0], axis=0))
        return jnp.einsum('lkbj,lkij->lbi', picked, to_float(operands[1]))
    return lax.map(per_box, (columns, blocks)).reshape(LEAVES, NRHS, 3 * LP)

def gather_flat(source, indices):
    chosen = jnp.take(source, indices, axis=0)
    chosen = jnp.transpose(chosen, (0, 2, 1, 3))
    return chosen.reshape(indices.shape[0], NRHS, indices.shape[1] * R)

def apply_operator(field, near_cols, near_blocks, col_basis, row_basis, leaf_far, leaf_coupling, leaf_transfer, box_far, box_coupling, box_transfer, coarse_far, coarse_coupling):
    field_bf = field.astype(jnp.bfloat16)
    near_sum = near_term(field_bf, near_cols, near_blocks)
    leaf_coef = jnp.einsum('lbj,lrj->lbr', to_float(field_bf), to_float(col_basis)).astype(jnp.bfloat16)
    leaf_blocks = leaf_transfer.reshape(BOXES, LD, R, R)
    box_coef = jnp.einsum('xlbr,xlrs->xbs', to_float(leaf_coef).reshape(BOXES, LD, NRHS, R), leaf_blocks, precision=highest).astype(jnp.bfloat16)
    parent_part = jnp.einsum('xbr,xrs->xbs', to_float(box_coef), box_transfer, precision=highest).astype(jnp.bfloat16)
    group_coef = to_float(parent_part).reshape(GROUPS, BOX_GROUP, NRHS, R).sum(axis=1).astype(jnp.bfloat16)
    leaf_field = jnp.einsum('lbm,lrm->lbr', to_float(gather_flat(leaf_coef, leaf_far)), to_float(leaf_coupling))
    box_field = jnp.einsum('xbm,xrm->xbr', to_float(gather_flat(box_coef, box_far)), to_float(box_coupling))
    group_field = jnp.einsum('gbm,grm->gbr', to_float(gather_flat(group_coef, coarse_far)), to_float(coarse_coupling))
    spread = jnp.repeat(group_field, BOX_GROUP, axis=0)
    box_local = box_field + jnp.einsum('xbs,xrs->xbr', spread, box_transfer, precision=highest)
    leaf_local = leaf_field + jnp.einsum('xbs,xlrs->xlbr', box_local, leaf_blocks, precision=highest).reshape(LEAVES, NRHS, R)
    leaf_local = leaf_local.astype(jnp.bfloat16)
    far_sum = jnp.einsum('lbr,lrj->lbj', to_float(leaf_local), to_float(row_basis))
    return 0.5 * field + near_sum + far_sum

def mean_product(left, right):
    return lax.optimization_barrier(jnp.mean(left * right, axis=(0, 2)))

def spread_rhs(values):
    return values[None, :, None]

def reference(vector, near_cols, near_blocks, col_basis, row_basis, leaf_far, leaf_coupling, leaf_transfer, box_far, box_coupling, box_transfer, coarse_far, coarse_coupling):

    def operator(field):
        return apply_operator(field, near_cols, near_blocks, col_basis, row_basis, leaf_far, leaf_coupling, leaf_transfer, box_far, box_coupling, box_transfer, coarse_far, coarse_coupling)
    norm_first = jnp.sqrt(mean_product(vector, vector) + epsilon)
    first_basis = vector / spread_rhs(norm_first)
    image_one = operator(first_basis)
    proj_first = mean_product(first_basis, image_one)
    image_one = image_one - spread_rhs(proj_first) * first_basis
    norm_image = jnp.sqrt(mean_product(image_one, image_one) + epsilon)
    basis = image_one / spread_rhs(norm_image)
    remainder = operator(basis)
    proj_second = mean_product(first_basis, remainder)
    remainder = remainder - spread_rhs(proj_second) * first_basis
    proj_basis = mean_product(basis, remainder)
    remainder = remainder - spread_rhs(proj_basis) * basis
    norm_last = jnp.sqrt(mean_product(remainder, remainder) + epsilon)
    hessenberg = jnp.stack([proj_first, norm_image, proj_second, proj_basis, norm_last], axis=1)
    return (basis, remainder, hessenberg)
```

```python
import jax
import jax.numpy as jnp
from jax import lax
from jax.experimental import pallas as pl
from jax.experimental.pallas import tpu as pltpu
from jax.sharding import Mesh
from jax.sharding import PartitionSpec as P

R = 32
GRP = ("grp_0", "grp_1")
ROWS = ("rows_0", "rows_1", "rows_2")
ROWS_GRP = ("rows_0", "rows_1", "rows_2", "grp_0", "grp_1")
BF = jnp.bfloat16
F32 = jnp.float32

epsilon = 1e-06
SMALL = 2.0**-40
SWITCH = 2.0**-20

NT = (((1,), (1,)), ((), ()))
NN = (((1,), (0,)), ((), ()))

VMEM = pl.BlockSpec(memory_space=pltpu.VMEM)
SMEM = pl.BlockSpec(memory_space=pltpu.SMEM)


def dot(left, right, dims=NN):
    return lax.dot_general(left, right, dims, preferred_element_type=F32)


def row_col(shape):
    return (
        lax.broadcasted_iota(jnp.int32, shape, 0),
        lax.broadcasted_iota(jnp.int32, shape, 1),
    )


def diagonal(leaves, nrhs):
    row, col = row_col((leaves * nrhs, leaves * R))
    return row // nrhs == col // R


def over_leaves(array, leaves):
    step = array.shape[0] // leaves
    total = array[:step]
    for l in range(1, leaves):
        total = total + array[l * step : (l + 1) * step]
    return total


def coefficients(field_bf, col_basis, leaf_transfer, box_transfer, packet_ref, parent_ref):
    leaves = col_basis.shape[0]
    nrhs = field_bf.shape[0] // leaves
    full = dot(field_bf, col_basis.reshape(leaves * R, -1), NT)
    leaf = over_leaves(jnp.where(diagonal(leaves, nrhs), full, 0.0), leaves).astype(BF)
    transfer = leaf_transfer.reshape(leaves * R, R).astype(BF)
    box = dot(leaf, transfer).astype(BF)
    parent = dot(box, box_transfer.astype(BF)).astype(BF)
    row, col = row_col((R, leaves * R))
    spread = dot(box, (row == col).astype(BF)).astype(BF)
    packet = jnp.concatenate([leaf, spread], axis=0)
    packet_ref[...] = jnp.broadcast_to(packet[None], packet_ref.shape)
    tiled = dot(parent, (row == col % R).astype(BF))
    per_row = nrhs * R // (leaves * R)
    row, col = row_col((nrhs, leaves * R))
    tiled = jnp.where(row // per_row == col // R, tiled, 0.0).astype(BF)
    row, col = row_col((8, nrhs))
    dense = dot((row == col % per_row).astype(BF), tiled).astype(BF)[:per_row]
    parent_ref[...] = jnp.broadcast_to(dense[None], parent_ref.shape)


def start_kernel(vector, col_basis, leaf_transfer, box_transfer, field_ref, packet_ref, parent_ref):
    leaves, nrhs, width = vector.shape
    field = vector[...].reshape(leaves * nrhs, width).astype(BF)
    field_ref[...] = field
    coefficients(
        field, col_basis[...], leaf_transfer[...], box_transfer[0], packet_ref, parent_ref
    )


def near_kernel(near_cols, low, field, high, blocks, out, window):
    nrhs = out.shape[0]
    leaves = field.shape[0] // nrhs
    leaf = pl.program_id(0)

    @pl.when(leaf == 0)
    def _():
        for i, part in enumerate((low, field, high)):
            window[i * leaves : (i + 1) * leaves] = part[...].reshape(leaves, nrhs, -1)

    base = device_index() * leaves - leaves
    total = None
    for k in range(blocks.shape[1]):
        picked = window[near_cols[leaf, k] - base]
        term = dot(picked, blocks[0, k], NT)
        total = term if total is None else total + term
    out[...] = total


def device_index():
    index = lax.axis_index(ROWS_GRP[0])
    for axis in ROWS_GRP[1:]:
        index = index * lax.axis_size(axis) + lax.axis_index(axis)
    return index


def row_index():
    index = lax.axis_index(ROWS[0])
    for axis in ROWS[1:]:
        index = index * lax.axis_size(axis) + lax.axis_index(axis)
    return index


def fine_kernel(
    leaf_far, box_far, low, own, high, leaf_coupling, box_coupling, leaf_out, box_out, window
):
    group = own.shape[0]
    nrhs = box_out.shape[0]
    lanes = own.shape[2]
    leaves, kf = leaf_far.shape
    for i, part in enumerate((low, own, high)):
        window[i * group : (i + 1) * group] = part[...]
    first_box = (row_index() - 1) * group
    first_leaf = first_box * leaves
    _, col = row_col((nrhs, lanes))
    block = col // R
    per_tile = lanes // R
    rows = []
    for l in range(leaves):
        tiles = []
        for t in range(kf // per_tile):
            tile = jnp.zeros((nrhs, lanes), F32)
            for i in range(per_tile):
                index = leaf_far[l, t * per_tile + i] - first_leaf
                box = index // leaves
                item = index - box * leaves
                values = window[box, :nrhs].astype(F32)
                shift = lax.rem(i - item + per_tile, per_tile) * R
                values = pltpu.roll(values, shift, 1)
                tile = jnp.where(block == i, values, tile)
            tiles.append(tile.astype(BF))
        rows.append(jnp.concatenate(tiles, axis=1))
    gathered = jnp.concatenate(rows, axis=0)
    leaf_out[...] = dot(gathered, leaf_coupling[...].reshape(leaves * R, -1), NT)
    tile = jnp.zeros((nrhs, lanes), F32)
    for k in range(box_far.shape[1]):
        values = window[box_far[0, k] - first_box, nrhs:].astype(F32)
        if k:
            values = pltpu.roll(values, k * R, 1)
        tile = tile + values
    box_out[...] = dot(tile.astype(BF), box_coupling[0], NT)


def downward(
    coarse_far, parents, near, leaf_field, box_field, coarse_coupling, box_transfer,
    leaf_transfer, row_basis, stack,
):
    leaves = row_basis.shape[0]
    nrhs = near.shape[0] // leaves
    group = 4
    kc = coarse_far.shape[1]
    per_row, lanes = parents.shape[1:]
    for k in range(kc):
        first = coarse_far[0, k] * group
        total = parents[first].astype(F32)
        for j in range(1, group):
            total = total + parents[first + j].astype(F32)
        stack[k * per_row : (k + 1) * per_row] = total
    dense = stack[...].astype(BF)
    row, col = row_col((kc * nrhs, kc * per_row))
    pick = (row // nrhs == col // per_row) & (row % per_row == col % per_row)
    wide = dot(pick.astype(BF), dense)
    row, col = row_col((kc * nrhs, lanes))
    wide = jnp.where(row % nrhs // per_row == col // R, wide, 0.0)
    half = wide + pltpu.roll(wide, 2 * R, 1)
    wide = half + pltpu.roll(half, R, 1)
    wide = jnp.where(row // nrhs == col // R, wide, 0.0)
    gathered = over_leaves(wide, kc).astype(BF)
    group_field = dot(gathered, coarse_coupling[0], NT)
    box_local = box_field[...] + dot(group_field.astype(BF), box_transfer[0].astype(BF), NT)
    transfer = leaf_transfer[...].reshape(leaves * R, R).astype(BF)
    shared = dot(box_local.astype(BF), transfer, NT)
    local = leaf_field[...] + jnp.concatenate([shared] * leaves, axis=0)
    local = jnp.where(diagonal(leaves, nrhs), local, 0.0).astype(BF)
    return near[...] + dot(local, row_basis[...].reshape(leaves * R, -1))


def middle_kernel(
    coarse_far, parents, near, leaf_field, box_field, coarse_coupling, box_transfer,
    leaf_transfer, row_basis, col_basis, image_ref, field_ref, packet_ref, parent_ref, stack,
):
    image = downward(
        coarse_far, parents, near, leaf_field, box_field, coarse_coupling, box_transfer,
        leaf_transfer, row_basis, stack,
    )
    image_ref[...] = image
    field = image.astype(BF)
    field_ref[...] = field
    coefficients(
        field, col_basis[...], leaf_transfer[...], box_transfer[0], packet_ref, parent_ref
    )


def products_kernel(
    coarse_far, parents, near, leaf_field, box_field, coarse_coupling, box_transfer,
    leaf_transfer, row_basis, vector, image, second_ref, sums_ref, stack,
):
    leaves, nrhs, width = vector.shape
    second = downward(
        coarse_far, parents, near, leaf_field, box_field, coarse_coupling, box_transfer,
        leaf_transfer, row_basis, stack,
    )
    second_ref[...] = second
    first = vector[...].reshape(leaves * nrhs, width)
    middle = image[...]
    small = second * SMALL
    pairs = (
        (first, first), (first, middle), (middle, middle), (first, second),
        (middle, second), (second, second), (middle, small), (small, small),
    )
    parts = []
    for left, right in pairs:
        product = over_leaves(left * right, leaves)
        part = product[:, :128]
        for i in range(1, width // 128):
            part = part + product[:, i * 128 : (i + 1) * 128]
        parts.append(part)
    table = jnp.concatenate(parts, axis=0)
    sums = jnp.sum(table.T, axis=0, keepdims=True)
    sums_ref[...] = jnp.broadcast_to(sums[None], sums_ref.shape)


def finish_kernel(sums, vector, image, second, basis_ref, remainder_ref, hessenberg_ref):
    leaves, nrhs, width = vector.shape
    count = sums.shape[0] * leaves * width
    total = jnp.sum(sums[...], axis=0)
    row, col = row_col((nrhs, total.shape[1]))
    total = jnp.broadcast_to(total, (nrhs, total.shape[1]))

    def mean(i):
        own = jnp.where(col == i * nrhs + row, total, 0.0)
        return jnp.sum(own, axis=1, keepdims=True) / count

    vv, vu, uu, vz = mean(0), mean(1), mean(2), mean(3)
    large = mean(7) > SWITCH
    uz = jnp.where(large, mean(6), mean(4))
    zz = jnp.where(large, mean(7), mean(5))
    unit = jnp.where(large, 1.0 / SMALL, 1.0)
    square_first = vv + epsilon
    norm_first = jnp.sqrt(square_first)
    ratio = vu / square_first
    proj_first = 0.5 * vv / square_first + ratio
    shift = proj_first - 0.5
    square_image = (uu - 2.0 * shift * vu + shift * shift * vv) / square_first
    norm_image = jnp.sqrt(square_image + epsilon)
    scale = 1.0 / (norm_first * norm_image)
    on_z = scale * unit
    on_u = scale * (0.5 - shift)
    on_v = -0.5 * shift * scale
    v_with = scale * vz + on_u * vu + on_v * vv
    u_with = on_z * uz + on_u * uu + on_v * vu
    proj_second = v_with / norm_first
    cross = scale * (vu - shift * vv) / norm_first
    proj_basis = scale * u_with - scale * shift * v_with - proj_second * cross
    on_u = on_u - proj_basis * scale
    on_v = on_v - proj_second / norm_first + proj_basis * scale * shift
    square_last = (
        on_z * (on_z * zz)
        + 2.0 * on_u * (on_z * uz)
        + 2.0 * on_v * (scale * vz)
        + on_u * (on_u * uu)
        + 2.0 * on_v * (on_u * vu)
        + on_v * (on_v * vv)
    )
    norm_last = jnp.sqrt(square_last + epsilon)
    for l in range(leaves):
        rows = pl.ds(l * nrhs, nrhs)
        v = vector[l]
        u = image[rows, :]
        basis_ref[l] = scale * u - (scale * shift) * v
        remainder_ref[l] = scale * second[rows, :] + on_u * u + on_v * v
    row, col = row_col((nrhs, 128))
    table = jnp.zeros((nrhs, 128), F32)
    for i, entry in enumerate((proj_first, norm_image, proj_second, proj_basis, norm_last)):
        table = jnp.where(col == i, entry, table)
    hessenberg_ref[...] = table[:, :5]


def shards(
    vector,
    near_cols,
    near_blocks,
    col_basis,
    row_basis,
    leaf_far,
    leaf_coupling,
    leaf_transfer,
    box_far,
    box_coupling,
    box_transfer,
    coarse_far,
    coarse_coupling,
):
    leaves, nrhs, width = vector.shape
    group = lax.axis_size(GRP)
    rows = lax.axis_size(ROWS)
    devices = rows * group
    kn = near_cols.shape[1]
    lanes = leaves * R
    flat = leaves * nrhs
    dense = nrhs * R // lanes
    shape = jax.ShapeDtypeStruct

    upward_out = (
        shape((flat, width), BF),
        shape((group, 2 * nrhs, lanes), BF),
        shape((devices, dense, lanes), BF),
    )

    def exchange(field, packet, parent):
        parents = lax.all_to_all(parent, ROWS_GRP, 0, 0, tiled=True)
        up = [(i, i + 1) for i in range(devices - 1)]
        down = [(b, a) for a, b in up]
        low_field = lax.ppermute(field, ROWS_GRP, up)
        high_field = lax.ppermute(field, ROWS_GRP, down)
        own = lax.all_to_all(packet, GRP, 0, 0, tiled=True)
        up = [(i, i + 1) for i in range(rows - 1)]
        down = [(b, a) for a, b in up]
        low = lax.ppermute(own, ROWS, up)
        high = lax.ppermute(own, ROWS, down)
        whole = pl.BlockSpec((flat, width), lambda l: (0, 0))
        near = pl.pallas_call(
            near_kernel,
            grid=(leaves,),
            in_specs=[
                SMEM, whole, whole, whole,
                pl.BlockSpec((1, kn, width, width), lambda l: (l, 0, 0, 0)),
            ],
            out_specs=pl.BlockSpec((nrhs, width), lambda l: (l, 0)),
            out_shape=shape((flat, width), F32),
            scratch_shapes=[pltpu.VMEM((3 * leaves, nrhs, width), BF)],
            name="near",
        )(near_cols, low_field, field, high_field, near_blocks)
        leaf_field, box_field = pl.pallas_call(
            fine_kernel,
            in_specs=[SMEM, SMEM] + [VMEM] * 5,
            out_specs=(VMEM, VMEM),
            out_shape=(shape((flat, lanes), F32), shape((nrhs, R), F32)),
            scratch_shapes=[pltpu.VMEM((3 * group, 2 * nrhs, lanes), BF)],
            name="fine",
        )(leaf_far, box_far, low, own, high, leaf_coupling, box_coupling)
        return (
            coarse_far, parents, near, leaf_field, box_field, coarse_coupling, box_transfer,
            leaf_transfer, row_basis,
        )

    stack = pltpu.VMEM((coarse_far.shape[1] * dense, lanes), F32)
    upward = pl.pallas_call(
        start_kernel,
        in_specs=[VMEM] * 4,
        out_specs=(VMEM,) * 3,
        out_shape=upward_out,
        name="start",
    )(vector, col_basis, leaf_transfer, box_transfer)
    image, *upward = pl.pallas_call(
        middle_kernel,
        in_specs=[SMEM] + [VMEM] * 9,
        out_specs=(VMEM,) * 4,
        out_shape=(shape((flat, width), F32), *upward_out),
        scratch_shapes=[stack],
        name="middle",
    )(*exchange(*upward), col_basis)
    second, sums = pl.pallas_call(
        products_kernel,
        in_specs=[SMEM] + [VMEM] * 10,
        out_specs=(VMEM,) * 2,
        out_shape=(shape((flat, width), F32), shape((devices, 1, 8 * nrhs), F32)),
        scratch_shapes=[stack],
        name="products",
    )(*exchange(*upward), vector, image)
    sums = lax.all_to_all(sums, ROWS_GRP, 0, 0, tiled=True)
    return pl.pallas_call(
        finish_kernel,
        in_specs=[VMEM] * 4,
        out_specs=(VMEM,) * 3,
        out_shape=(
            shape(vector.shape, F32),
            shape(vector.shape, F32),
            shape((nrhs, 5), F32),
        ),
        name="finish",
    )(sums, vector, image, second)


def solution(mesh):
    finer = Mesh(
        mesh.devices.reshape(4, 4, 4, 2, 2), ("rows_0", "rows_1", "rows_2", "grp_0", "grp_1")
    )
    placed = (
        P(ROWS_GRP, None, None),
        P(ROWS_GRP, None),
        P(ROWS_GRP, None, None, None),
        P(ROWS_GRP, None, None),
        P(ROWS_GRP, None, None),
        P(ROWS_GRP, None),
        P(ROWS_GRP, None, None),
        P(ROWS_GRP, None, None),
        P(ROWS_GRP, None),
        P(ROWS_GRP, None, None),
        P(ROWS_GRP, None, None),
        P(ROWS, None),
        P(ROWS, None, None),
    )
    return jax.shard_map(
        shards,
        mesh=finer,
        in_specs=placed,
        out_specs=(P(ROWS_GRP, None, None), P(ROWS_GRP, None, None), P()),
        check_vma=False,
    )
```

```python
import jax
import jax.numpy as jnp
from jax import lax
from jax.experimental import pallas as pl
from jax.experimental.pallas import tpu as pltpu
from jax.sharding import Mesh
from jax.sharding import PartitionSpec as P

R = 32
GRP = ("grp_0", "grp_1")
ROWS = ("rows_0", "rows_1", "rows_2")
ROWS_GRP = ("rows_0", "rows_1", "rows_2", "grp_0", "grp_1")
BF = jnp.bfloat16
F32 = jnp.float32

epsilon = 1e-06
SMALL = 2.0**-40
SWITCH = 2.0**-20
LIMIT = 16 * 2**20

NT = (((1,), (1,)), ((), ()))
NN = (((1,), (0,)), ((), ()))

VMEM = pl.BlockSpec(memory_space=pltpu.VMEM)
SMEM = pl.BlockSpec(memory_space=pltpu.SMEM)


def dot(left, right, dims=NN):
    return lax.dot_general(left, right, dims, preferred_element_type=F32)


def row_col(shape):
    return (
        lax.broadcasted_iota(jnp.int32, shape, 0),
        lax.broadcasted_iota(jnp.int32, shape, 1),
    )


def diagonal(leaves, nrhs):
    row, col = row_col((leaves * nrhs, leaves * R))
    return row // nrhs == col // R


def over_leaves(array, leaves):
    step = array.shape[0] // leaves
    total = array[:step]
    for l in range(1, leaves):
        total = total + array[l * step : (l + 1) * step]
    return total


def coefficients(field_bf, col_basis, leaf_transfer, box_transfer, packet_ref):
    leaves = col_basis.shape[0]
    lanes = leaves * R
    nrhs = field_bf.shape[0] // leaves
    full = dot(field_bf, col_basis.reshape(lanes, -1), NT)
    leaf = over_leaves(jnp.where(diagonal(leaves, nrhs), full, 0.0), leaves).astype(BF)
    box = dot(leaf, leaf_transfer.reshape(lanes, R).astype(BF)).astype(BF)
    parent = dot(box, box_transfer.astype(BF)).astype(BF)
    row, col = row_col((R, lanes))
    both = dot(box, (row == col).astype(BF)) + dot(parent, (row + R == col).astype(BF))
    blocks = []
    for l in range(leaves):
        for t in range(field_bf.shape[1] // lanes):
            blocks.append(field_bf[l * nrhs : (l + 1) * nrhs, t * lanes : (t + 1) * lanes])
    blocks += [leaf, both.astype(BF)]
    packet = jnp.concatenate(blocks, axis=0)
    packet_ref[...] = jnp.broadcast_to(packet[None], packet_ref.shape)


def start_kernel(vector, col_basis, leaf_transfer, box_transfer, packet_ref):
    leaves, nrhs, width = vector.shape
    field = vector[...].reshape(leaves * nrhs, width).astype(BF)
    coefficients(field, col_basis[...], leaf_transfer[...], box_transfer[0], packet_ref)


def group_kernel(own, side_ref, parent_ref):
    group, size, lanes = own.shape
    nrhs = 16
    fields = size - 2 * nrhs
    total = own[0, fields + nrhs :].astype(F32)
    for j in range(1, group):
        total = total + own[j, fields + nrhs :].astype(F32)
    total = total.astype(BF)
    row, col = row_col((lanes, lanes))
    tiled = dot(total, ((row // R == 1) & (row % R == col % R)).astype(BF))
    per_row = parent_ref.shape[1]
    row, col = row_col((nrhs, lanes))
    tiled = jnp.where(row // per_row == col // R, tiled, 0.0).astype(BF)
    row, col = row_col((8, nrhs))
    dense = dot((row == col % per_row).astype(BF), tiled).astype(BF)[:per_row]
    parent_ref[...] = jnp.broadcast_to(dense[None], parent_ref.shape)
    position = lax.axis_index(GRP[0]) * lax.axis_size(GRP[1]) + lax.axis_index(GRP[1])
    side_ref[:fields] = own[position, :fields]
    for j in range(group):
        side_ref[fields + j * 2 * nrhs : fields + (j + 1) * 2 * nrhs] = own[j, fields:]


def row_index():
    index = lax.axis_index(ROWS[0])
    for axis in ROWS[1:]:
        index = index * lax.axis_size(axis) + lax.axis_index(axis)
    return index


def near_kernel(near_cols, low, own, high, blocks, out, window, weights, sems):
    leaves, kn, width, _ = blocks.shape
    nrhs = out.shape[0] // leaves
    group = own.shape[0]
    fields = window.shape[1]
    copies = [
        pltpu.make_async_copy(blocks.at[l], weights.at[l], sems.at[l]) for l in range(leaves)
    ]
    for copy in copies:
        copy.start()
    window[0] = low[:fields]
    for j in range(group):
        window[j + 1] = own[j, :fields]
    window[group + 1] = high[:fields]
    base = (row_index() * group - 1) * leaves
    tiles = fields // leaves // nrhs
    for l in range(leaves):
        picked = []
        for k in range(kn):
            index = near_cols[l, k] - base
            device = index // leaves
            first = (index - device * leaves) * (tiles * nrhs)
            picked += [
                window[device, pl.ds(pl.multiple_of(first + t * nrhs, nrhs), nrhs)]
                for t in range(tiles)
            ]
        copies[l].wait()
        total = None
        for k in range(kn):
            part = jnp.concatenate(picked[k * tiles : (k + 1) * tiles], axis=1)
            term = dot(part, weights[l, k], NT)
            total = term if total is None else total + term
        out[l * nrhs : (l + 1) * nrhs] = total


def fine_kernel(
    leaf_far, box_far, low, own, high, leaf_coupling, box_coupling, leaf_out, box_out, window
):
    group, size, lanes = own.shape
    nrhs = box_out.shape[0]
    leaves, kf = leaf_far.shape
    fields = size - 2 * nrhs
    for j in range(group):
        rows = slice(fields + j * 2 * nrhs, fields + (j + 1) * 2 * nrhs)
        window[j] = low[rows]
        window[group + j] = own[j, fields:]
        window[2 * group + j] = high[rows]
    first_box = (row_index() - 1) * group
    first_leaf = first_box * leaves
    _, col = row_col((nrhs, lanes))
    block = col // R
    per_tile = lanes // R
    rows = []
    for l in range(leaves):
        tiles = []
        for t in range(kf // per_tile):
            tile = jnp.zeros((nrhs, lanes), F32)
            for i in range(per_tile):
                index = leaf_far[l, t * per_tile + i] - first_leaf
                box = index // leaves
                item = index - box * leaves
                values = window[box, :nrhs].astype(F32)
                shift = lax.rem(i - item + per_tile, per_tile) * R
                values = pltpu.roll(values, shift, 1)
                tile = jnp.where(block == i, values, tile)
            tiles.append(tile.astype(BF))
        rows.append(jnp.concatenate(tiles, axis=1))
    gathered = jnp.concatenate(rows, axis=0)
    leaf_out[...] = dot(gathered, leaf_coupling[...].reshape(leaves * R, -1), NT)
    tile = jnp.zeros((nrhs, lanes), F32)
    for k in range(box_far.shape[1]):
        values = window[box_far[0, k] - first_box, nrhs:].astype(F32)
        if k:
            values = pltpu.roll(values, k * R, 1)
        tile = jnp.where(block == k, values, tile)
    box_out[...] = dot(tile.astype(BF), box_coupling[0], NT)


def downward(
    coarse_far, parents, near, leaf_field, box_field, coarse_coupling, box_transfer,
    leaf_transfer, row_basis, stack,
):
    leaves = row_basis.shape[0]
    nrhs = near.shape[0] // leaves
    kc = coarse_far.shape[1]
    per_row, lanes = parents.shape[1:]
    for k in range(kc):
        stack[k * per_row : (k + 1) * per_row] = parents[coarse_far[0, k]].astype(F32)
    dense = stack[...].astype(BF)
    row, col = row_col((kc * nrhs, kc * per_row))
    pick = (row // nrhs == col // per_row) & (row % per_row == col % per_row)
    wide = dot(pick.astype(BF), dense)
    row, col = row_col((kc * nrhs, lanes))
    wide = jnp.where(row % nrhs // per_row == col // R, wide, 0.0)
    half = wide + pltpu.roll(wide, 2 * R, 1)
    wide = half + pltpu.roll(half, R, 1)
    wide = jnp.where(row // nrhs == col // R, wide, 0.0)
    gathered = over_leaves(wide, kc).astype(BF)
    group_field = dot(gathered, coarse_coupling[0], NT)
    box_local = box_field[...] + dot(group_field.astype(BF), box_transfer[0].astype(BF), NT)
    transfer = leaf_transfer[...].reshape(leaves * R, R).astype(BF)
    shared = dot(box_local.astype(BF), transfer, NT)
    local = leaf_field[...] + jnp.concatenate([shared] * leaves, axis=0)
    local = jnp.where(diagonal(leaves, nrhs), local, 0.0).astype(BF)
    return near[...] + dot(local, row_basis[...].reshape(leaves * R, -1))


def middle_kernel(
    coarse_far, parents, near, leaf_field, box_field, coarse_coupling, box_transfer,
    leaf_transfer, row_basis, col_basis, image_ref, packet_ref, stack,
):
    image = downward(
        coarse_far, parents, near, leaf_field, box_field, coarse_coupling, box_transfer,
        leaf_transfer, row_basis, stack,
    )
    image_ref[...] = image
    coefficients(
        image.astype(BF), col_basis[...], leaf_transfer[...], box_transfer[0], packet_ref
    )


def products_kernel(
    coarse_far, parents, near, leaf_field, box_field, coarse_coupling, box_transfer,
    leaf_transfer, row_basis, vector, image, second_ref, sums_ref, stack,
):
    leaves, nrhs, width = vector.shape
    second = downward(
        coarse_far, parents, near, leaf_field, box_field, coarse_coupling, box_transfer,
        leaf_transfer, row_basis, stack,
    )
    second_ref[...] = second
    first = vector[...].reshape(leaves * nrhs, width)
    middle = image[...]
    small = second * SMALL
    pairs = (
        (first, first), (first, middle), (middle, middle), (first, second),
        (middle, second), (second, second), (middle, small), (small, small),
    )
    parts = []
    for left, right in pairs:
        product = over_leaves(left * right, leaves)
        part = product[:, :128]
        for i in range(1, width // 128):
            part = part + product[:, i * 128 : (i + 1) * 128]
        parts.append(part)
    table = jnp.concatenate(parts, axis=0)
    sums = jnp.sum(table.T, axis=0, keepdims=True)
    sums_ref[...] = jnp.broadcast_to(sums[None], sums_ref.shape)


def finish_kernel(sums, vector, image, second, basis_ref, remainder_ref, hessenberg_ref):
    leaves, nrhs, width = vector.shape
    count = sums.shape[0] * leaves * width
    total = jnp.sum(sums[...], axis=0)
    row, col = row_col((nrhs, total.shape[1]))
    total = jnp.broadcast_to(total, (nrhs, total.shape[1]))

    def mean(i):
        own = jnp.where(col == i * nrhs + row, total, 0.0)
        return jnp.sum(own, axis=1, keepdims=True) / count

    vv, vu, uu, vz = mean(0), mean(1), mean(2), mean(3)
    large = mean(7) > SWITCH
    uz = jnp.where(large, mean(6), mean(4))
    zz = jnp.where(large, mean(7), mean(5))
    unit = jnp.where(large, 1.0 / SMALL, 1.0)
    square_first = vv + epsilon
    norm_first = jnp.sqrt(square_first)
    ratio = vu / square_first
    proj_first = 0.5 * vv / square_first + ratio
    shift = proj_first - 0.5
    square_image = (uu - 2.0 * shift * vu + shift * shift * vv) / square_first
    norm_image = jnp.sqrt(square_image + epsilon)
    scale = 1.0 / (norm_first * norm_image)
    on_z = scale * unit
    on_u = scale * (0.5 - shift)
    on_v = -0.5 * shift * scale
    v_with = scale * vz + on_u * vu + on_v * vv
    u_with = on_z * uz + on_u * uu + on_v * vu
    proj_second = v_with / norm_first
    cross = scale * (vu - shift * vv) / norm_first
    proj_basis = scale * u_with - scale * shift * v_with - proj_second * cross
    on_u = on_u - proj_basis * scale
    on_v = on_v - proj_second / norm_first + proj_basis * scale * shift
    square_last = (
        on_z * (on_z * zz)
        + 2.0 * on_u * (on_z * uz)
        + 2.0 * on_v * (scale * vz)
        + on_u * (on_u * uu)
        + 2.0 * on_v * (on_u * vu)
        + on_v * (on_v * vv)
    )
    norm_last = jnp.sqrt(square_last + epsilon)
    for l in range(leaves):
        rows = pl.ds(l * nrhs, nrhs)
        v = vector[l]
        u = image[rows, :]
        basis_ref[l] = scale * u - (scale * shift) * v
        remainder_ref[l] = scale * second[rows, :] + on_u * u + on_v * v
    entries = (proj_first, norm_image, proj_second, proj_basis, norm_last)
    row, col = row_col((nrhs, nrhs))
    for i, entry in enumerate(entries):
        line = jnp.sum(jnp.where(row == col, entry, 0.0), axis=0, keepdims=True)
        hessenberg_ref[i : i + 1] = line


def shards(
    vector,
    near_cols,
    near_blocks,
    col_basis,
    row_basis,
    leaf_far,
    leaf_coupling,
    leaf_transfer,
    box_far,
    box_coupling,
    box_transfer,
    coarse_far,
    coarse_coupling,
):
    leaves, nrhs, width = vector.shape
    group = lax.axis_size(GRP)
    rows = lax.axis_size(ROWS)
    devices = rows * group
    kn = near_cols.shape[1]
    lanes = leaves * R
    flat = leaves * nrhs
    dense = nrhs * R // lanes
    tiles = width // lanes
    size = (leaves * tiles + 2) * nrhs
    side = (leaves * tiles + 2 * group) * nrhs
    params = pltpu.CompilerParams(vmem_limit_bytes=LIMIT)

    given = {id(a) for a in (
        vector, near_cols, near_blocks, col_basis, row_basis, leaf_far, leaf_coupling,
        leaf_transfer, box_far, box_coupling, box_transfer, coarse_far, coarse_coupling,
    )}

    def placed(arrays):
        return [
            pltpu.with_memory_space_constraint(a, pltpu.HBM if id(a) in given else pltpu.VMEM)
            for a in arrays
        ]

    def made(*dims, dtype=F32):
        return pltpu.VMEM(dims, dtype)

    def call(kernel, inputs, outs, smem=(), hbm=(), scratch=()):
        specs = [SMEM] * len(smem) + [VMEM] * len(inputs)
        specs += [pl.BlockSpec(memory_space=pl.ANY)] * len(hbm)
        return pl.pallas_call(
            kernel,
            in_specs=specs,
            out_specs=[VMEM] * len(outs),
            out_shape=outs,
            scratch_shapes=scratch,
            compiler_params=params,
            name=kernel.__name__,
        )(*placed(smem), *placed(inputs), *placed(hbm))

    step = [
        (i, (i // group + 1) * group + (i + 1) % group) for i in range(devices - group)
    ]

    def exchange(packet):
        own = lax.all_to_all(packet, GRP, 0, 0, tiled=True)
        sides, parent = call(
            group_kernel, [own], [made(side, lanes, dtype=BF), made(rows, dense, lanes, dtype=BF)]
        )
        low = lax.ppermute(sides, ROWS_GRP, step)
        high = lax.ppermute(sides, ROWS_GRP, [(b, a) for a, b in step])
        parents = lax.all_to_all(parent, ROWS, 0, 0, tiled=True)
        (near,) = call(
            near_kernel,
            [low, own, high],
            [made(flat, width)],
            smem=[near_cols],
            hbm=[near_blocks],
            scratch=[
                pltpu.VMEM((group + 2, leaves * tiles * nrhs, lanes), BF),
                pltpu.VMEM((leaves, kn, width, width), BF),
                pltpu.SemaphoreType.DMA((leaves,)),
            ],
        )
        leaf_field, box_field = call(
            fine_kernel,
            [low, own, high, leaf_coupling, box_coupling],
            [made(flat, lanes), made(nrhs, R)],
            smem=[leaf_far, box_far],
            scratch=[pltpu.VMEM((3 * group, 2 * nrhs, lanes), BF)],
        )
        return [
            parents, near, leaf_field, box_field, coarse_coupling, box_transfer, leaf_transfer,
            row_basis,
        ]

    packet_out = made(group, size, lanes, dtype=BF)
    stack = pltpu.VMEM((coarse_far.shape[1] * dense, lanes), F32)
    (packet,) = call(start_kernel, [vector, col_basis, leaf_transfer, box_transfer], [packet_out])
    image, packet = call(
        middle_kernel,
        exchange(packet) + [col_basis],
        [made(flat, width), packet_out],
        smem=[coarse_far],
        scratch=[stack],
    )
    second, sums = call(
        products_kernel,
        exchange(packet) + [vector, image],
        [made(flat, width), made(devices, 1, 8 * nrhs)],
        smem=[coarse_far],
        scratch=[stack],
    )
    sums = lax.all_to_all(sums, ROWS_GRP, 0, 0, tiled=True)
    shape = jax.ShapeDtypeStruct
    basis, remainder, hessenberg = call(
        finish_kernel,
        [sums, vector, image, second],
        [shape(vector.shape, F32), shape(vector.shape, F32), shape((5, nrhs), F32)],
    )
    return basis, remainder, hessenberg.T


def solution(mesh):
    finer = Mesh(
        mesh.devices.reshape(4, 4, 4, 2, 2), ("rows_0", "rows_1", "rows_2", "grp_0", "grp_1")
    )
    placed = (
        P(ROWS_GRP, None, None),
        P(ROWS_GRP, None),
        P(ROWS_GRP, None, None, None),
        P(ROWS_GRP, None, None),
        P(ROWS_GRP, None, None),
        P(ROWS_GRP, None),
        P(ROWS_GRP, None, None),
        P(ROWS_GRP, None, None),
        P(ROWS_GRP, None),
        P(ROWS_GRP, None, None),
        P(ROWS_GRP, None, None),
        P(ROWS, None),
        P(ROWS, None, None),
    )
    return jax.shard_map(
        shards,
        mesh=finer,
        in_specs=placed,
        out_specs=(P(ROWS_GRP, None, None), P(ROWS_GRP, None, None), P()),
        check_vma=False,
    )
```

```python
import jax
import jax.numpy as jnp
from jax import lax
from jax.experimental import pallas as pl
from jax.experimental.pallas import tpu as pltpu
from jax.sharding import Mesh
from jax.sharding import PartitionSpec as P


R = 32
GRP = ("grp_0", "grp_1")
ROWS = ("rows_0", "rows_1", "rows_2")
ROWS_GRP = ("rows_0", "rows_1", "rows_2", "grp_0", "grp_1")
BF = jnp.bfloat16
F32 = jnp.float32

epsilon = 1e-06
SMALL = 2.0**-40
SWITCH = 2.0**-20
LIMIT = 16 * 2**20

NT = (((1,), (1,)), ((), ()))
NN = (((1,), (0,)), ((), ()))

VMEM = pl.BlockSpec(memory_space=pltpu.VMEM)
SMEM = pl.BlockSpec(memory_space=pltpu.SMEM)


def dot(left, right, dims=NN):
    return lax.dot_general(left, right, dims, preferred_element_type=F32)


def row_col(shape):
    return (
        lax.broadcasted_iota(jnp.int32, shape, 0),
        lax.broadcasted_iota(jnp.int32, shape, 1),
    )


def diagonal(leaves, nrhs):
    row, col = row_col((leaves * nrhs, leaves * R))
    return row // nrhs == col // R


def over_leaves(array, leaves):
    step = array.shape[0] // leaves
    total = array[:step]
    for l in range(1, leaves):
        total = total + array[l * step : (l + 1) * step]
    return total


def coefficients(field_bf, col_basis, leaf_transfer, box_transfer, packet_ref):
    lanes = col_basis.shape[0]
    leaves = lanes // R
    nrhs = field_bf.shape[0] // leaves
    full = dot(field_bf, col_basis, NT)
    leaf = over_leaves(jnp.where(diagonal(leaves, nrhs), full, 0.0), leaves).astype(BF)
    box = dot(leaf, leaf_transfer).astype(BF)
    parent = dot(box, box_transfer).astype(BF)
    row, col = row_col((R, lanes))
    both = dot(box, (row == col).astype(BF)) + dot(parent, (row + R == col).astype(BF))
    blocks = []
    for l in range(leaves):
        for t in range(field_bf.shape[1] // lanes):
            blocks.append(field_bf[l * nrhs : (l + 1) * nrhs, t * lanes : (t + 1) * lanes])
    blocks += [leaf, both.astype(BF)]
    packet = jnp.concatenate(blocks, axis=0)
    packet_ref[...] = jnp.broadcast_to(packet[None], packet_ref.shape)


def start_kernel(vector, col_basis, leaf_transfer, box_transfer, packet_ref):
    leaves, nrhs, width = vector.shape
    field = vector[...].reshape(leaves * nrhs, width).astype(BF)
    coefficients(
        field,
        col_basis[...].reshape(leaves * R, width),
        leaf_transfer[...].reshape(leaves * R, R).astype(BF),
        box_transfer[0].astype(BF),
        packet_ref,
    )


def group_kernel(own, side_ref, parent_ref):
    group, size, lanes = own.shape
    nrhs = 16
    fields = size - 2 * nrhs
    total = own[0, fields + nrhs :].astype(F32)
    for j in range(1, group):
        total = total + own[j, fields + nrhs :].astype(F32)
    total = total.astype(BF)
    row, col = row_col((lanes, lanes))
    tiled = dot(total, ((row // R == 1) & (row % R == col % R)).astype(BF))
    per_row = parent_ref.shape[1]
    row, col = row_col((nrhs, lanes))
    tiled = jnp.where(row // per_row == col // R, tiled, 0.0).astype(BF)
    row, col = row_col((8, nrhs))
    dense = dot((row == col % per_row).astype(BF), tiled).astype(BF)[:per_row]
    parent_ref[...] = jnp.broadcast_to(dense[None], parent_ref.shape)
    side_ref[:fields] = own[position(), :fields]
    for j in range(group):
        side_ref[fields + j * 2 * nrhs : fields + (j + 1) * 2 * nrhs] = own[j, fields:]


def position():
    return lax.axis_index(GRP[0]) * lax.axis_size(GRP[1]) + lax.axis_index(GRP[1])


def row_index():
    index = lax.axis_index(ROWS[0])
    for axis in ROWS[1:]:
        index = index * lax.axis_size(axis) + lax.axis_index(axis)
    return index


def near_kernel(near_cols, own, side, blocks, out, window, weights, sems):
    leaves, kn, _, _ = blocks.shape
    nrhs = out.shape[0] // leaves
    group = own.shape[0]
    fields = window.shape[1]
    copies = [
        pltpu.make_async_copy(blocks.at[l], weights.at[l], sems.at[l]) for l in range(leaves)
    ]
    for copy in copies:
        copy.start()
    window[0] = side[:fields]
    for j in range(group):
        window[j + 1] = own[j, :fields]
    window[group + 1] = side[:fields]
    base = (row_index() * group - 1) * leaves
    tiles = fields // leaves // nrhs
    for l in range(leaves):
        picked = []
        for k in range(kn):
            index = near_cols[l, k] - base
            device = index // leaves
            first = (index - device * leaves) * (tiles * nrhs)
            picked += [
                window[device, pl.ds(pl.multiple_of(first + t * nrhs, nrhs), nrhs)]
                for t in range(tiles)
            ]
        copies[l].wait()
        total = None
        for k in range(kn):
            part = jnp.concatenate(picked[k * tiles : (k + 1) * tiles], axis=1)
            term = dot(part, weights[l, k], NT)
            total = term if total is None else total + term
        out[l * nrhs : (l + 1) * nrhs] = total


def fine_sums(
    leaf_far, box_far, own, side, other, leaf_coupling, box_coupling, leaf_transfer, out, window
):
    group, size, lanes = own.shape
    leaves, kf = leaf_far.shape
    nrhs = out.shape[0] // leaves
    fields = size - 2 * nrhs
    is_low = position() < group // 2
    side_slot = jnp.where(is_low, 0, 2 * group)
    other_slot = jnp.where(is_low, 2 * group, 0)
    for j in range(group):
        rows = slice(fields + j * 2 * nrhs, fields + (j + 1) * 2 * nrhs)
        window[side_slot + j] = side[rows]
        window[group + j] = own[j, fields:]
        window[other_slot + j] = other[rows]
    first_box = (row_index() - 1) * group
    first_leaf = first_box * leaves
    _, col = row_col((nrhs, lanes))
    block = col // R
    per_tile = lanes // R
    rows = []
    for l in range(leaves):
        tiles = []
        for t in range(kf // per_tile):
            tile = jnp.zeros((nrhs, lanes), F32)
            for i in range(per_tile):
                index = leaf_far[l, t * per_tile + i] - first_leaf
                box = index // leaves
                item = index - box * leaves
                values = window[box, :nrhs].astype(F32)
                shift = lax.rem(i - item + per_tile, per_tile) * R
                values = pltpu.roll(values, shift, 1)
                tile = jnp.where(block == i, values, tile)
            tiles.append(tile.astype(BF))
        rows.append(jnp.concatenate(tiles, axis=1))
    gathered = jnp.concatenate(rows, axis=0)
    leaf_field = dot(gathered, leaf_coupling[...].reshape(leaves * R, -1), NT)
    tile = jnp.zeros((nrhs, lanes), F32)
    for k in range(box_far.shape[1]):
        values = window[box_far[0, k] - first_box, nrhs:].astype(F32)
        if k:
            values = pltpu.roll(values, k * R, 1)
        tile = jnp.where(block == k, values, tile)
    box_field = dot(tile.astype(BF), box_coupling[0], NT)
    transfer = leaf_transfer[...].reshape(leaves * R, R)
    shared = lax.dot_general(
        box_field, transfer, NT, precision=lax.Precision.HIGHEST, preferred_element_type=F32
    )
    out[...] = leaf_field + jnp.concatenate([shared] * leaves, axis=0)


def fine_kernel(
    leaf_far, box_far, own, side, other, leaf_coupling, box_coupling, leaf_transfer, out, window
):
    fine_sums(
        leaf_far, box_far, own, side, other, leaf_coupling, box_coupling, leaf_transfer, out,
        window,
    )


def fine_and_stage_kernel(
    leaf_far, box_far, own, side, other, leaf_coupling, box_coupling, leaf_transfer,
    coarse_coupling, box_transfer, row_basis, col_basis, vector, out, coarse_out, down_out,
    row_out, col_out, leaf_out, box_out, vector_out, window,
):
    fine_sums(
        leaf_far, box_far, own, side, other, leaf_coupling, box_coupling, leaf_transfer, out,
        window,
    )
    transfer = leaf_transfer[...].reshape(leaf_out.shape)
    coarse_out[...] = coarse_coupling[0]
    down_out[...] = lax.dot_general(
        transfer, box_transfer[0], NN, precision=lax.Precision.HIGHEST,
        preferred_element_type=F32,
    ).astype(BF)
    row_out[...] = row_basis[...].reshape(row_out.shape)
    col_out[...] = col_basis[...].reshape(col_out.shape)
    leaf_out[...] = transfer.astype(BF)
    box_out[...] = box_transfer[0].astype(BF)
    vector_out[...] = vector[...]


def downward(coarse_far, parents, near, local_field, coarse_coupling, down, row_basis, stack):
    kc = coarse_far.shape[1]
    per_row, lanes = parents.shape[1:]
    leaves = lanes // R
    nrhs = near.shape[0] // leaves
    for k in range(kc):
        stack[k * per_row : (k + 1) * per_row] = parents[coarse_far[0, k]].astype(F32)
    dense = stack[...].astype(BF)
    row, col = row_col((kc * nrhs, kc * per_row))
    pick = (row // nrhs == col // per_row) & (row % per_row == col % per_row)
    wide = dot(pick.astype(BF), dense)
    row, col = row_col((kc * nrhs, lanes))
    wide = jnp.where(row % nrhs // per_row == col // R, wide, 0.0)
    half = wide + pltpu.roll(wide, 2 * R, 1)
    wide = half + pltpu.roll(half, R, 1)
    wide = jnp.where(row // nrhs == col // R, wide, 0.0)
    gathered = over_leaves(wide, kc).astype(BF)
    group_field = dot(gathered, coarse_coupling[...], NT)
    shared = dot(group_field.astype(BF), down[...], NT)
    local = local_field[...] + jnp.concatenate([shared] * leaves, axis=0)
    local = jnp.where(diagonal(leaves, nrhs), local, 0.0).astype(BF)
    return near[...] + dot(local, row_basis[...])


def middle_kernel(
    coarse_far, parents, near, local_field, coarse_coupling, down, row_basis, col_basis,
    leaf_transfer, box_transfer, image_ref, packet_ref, stack,
):
    image = downward(
        coarse_far, parents, near, local_field, coarse_coupling, down, row_basis, stack
    )
    image_ref[...] = image
    coefficients(
        image.astype(BF), col_basis[...], leaf_transfer[...], box_transfer[...], packet_ref
    )


def products_kernel(
    coarse_far, parents, near, local_field, coarse_coupling, down, row_basis, vector, image,
    second_ref, sums_ref, stack,
):
    leaves, nrhs, width = vector.shape
    second = downward(
        coarse_far, parents, near, local_field, coarse_coupling, down, row_basis, stack
    )
    second_ref[...] = second
    first = vector[...].reshape(leaves * nrhs, width)
    middle = image[...]
    small = second * SMALL
    pairs = (
        (first, first), (first, middle), (middle, middle), (first, second),
        (middle, second), (second, second), (middle, small), (small, small),
    )
    parts = []
    for left, right in pairs:
        product = over_leaves(left * right, leaves)
        part = product[:, :128]
        for i in range(1, width // 128):
            part = part + product[:, i * 128 : (i + 1) * 128]
        parts.append(part)
    table = jnp.concatenate(parts, axis=0)
    sums = jnp.sum(table.T, axis=0, keepdims=True)
    sums_ref[...] = jnp.broadcast_to(sums[None], sums_ref.shape)


def finish_kernel(sums, vector, image, second, basis_ref, remainder_ref, hessenberg_ref):
    leaves, nrhs, width = vector.shape
    count = sums.shape[0] * leaves * width
    total = jnp.sum(sums[...], axis=0)
    row, col = row_col((nrhs, total.shape[1]))
    total = jnp.broadcast_to(total, (nrhs, total.shape[1]))

    def mean(i):
        own = jnp.where(col == i * nrhs + row, total, 0.0)
        return jnp.sum(own, axis=1, keepdims=True) / count

    vv, vu, uu, vz = mean(0), mean(1), mean(2), mean(3)
    large = mean(7) > SWITCH
    uz = jnp.where(large, mean(6), mean(4))
    zz = jnp.where(large, mean(7), mean(5))
    unit = jnp.where(large, 1.0 / SMALL, 1.0)
    square_first = vv + epsilon
    norm_first = jnp.sqrt(square_first)
    ratio = vu / square_first
    proj_first = 0.5 * vv / square_first + ratio
    shift = proj_first - 0.5
    square_image = (uu - 2.0 * shift * vu + shift * shift * vv) / square_first
    norm_image = jnp.sqrt(square_image + epsilon)
    scale = 1.0 / (norm_first * norm_image)
    on_z = scale * unit
    on_u = scale * (0.5 - shift)
    on_v = -0.5 * shift * scale
    v_with = scale * vz + on_u * vu + on_v * vv
    u_with = on_z * uz + on_u * uu + on_v * vu
    proj_second = v_with / norm_first
    cross = scale * (vu - shift * vv) / norm_first
    proj_basis = scale * u_with - scale * shift * v_with - proj_second * cross
    on_u = on_u - proj_basis * scale
    on_v = on_v - proj_second / norm_first + proj_basis * scale * shift
    square_last = (
        on_z * (on_z * zz)
        + 2.0 * on_u * (on_z * uz)
        + 2.0 * on_v * (scale * vz)
        + on_u * (on_u * uu)
        + 2.0 * on_v * (on_u * vu)
        + on_v * (on_v * vv)
    )
    norm_last = jnp.sqrt(square_last + epsilon)
    for l in range(leaves):
        rows = pl.ds(l * nrhs, nrhs)
        v = vector[l]
        u = image[rows, :]
        basis_ref[l] = scale * u - (scale * shift) * v
        remainder_ref[l] = scale * second[rows, :] + on_u * u + on_v * v
    entries = (proj_first, norm_image, proj_second, proj_basis, norm_last)
    row, col = row_col((nrhs, nrhs))
    for i, entry in enumerate(entries):
        line = jnp.sum(jnp.where(row == col, entry, 0.0), axis=0, keepdims=True)
        hessenberg_ref[i : i + 1] = line


def shards(
    vector,
    near_cols,
    near_blocks,
    col_basis,
    row_basis,
    leaf_far,
    leaf_coupling,
    leaf_transfer,
    box_far,
    box_coupling,
    box_transfer,
    coarse_far,
    coarse_coupling,
):
    leaves, nrhs, width = vector.shape
    group = lax.axis_size(GRP)
    rows = lax.axis_size(ROWS)
    devices = rows * group
    kn = near_cols.shape[1]
    lanes = leaves * R
    flat = leaves * nrhs
    dense = nrhs * R // lanes
    tiles = width // lanes
    size = (leaves * tiles + 2) * nrhs
    side = (leaves * tiles + 2 * group) * nrhs
    params = pltpu.CompilerParams(vmem_limit_bytes=LIMIT)

    given = {id(a) for a in (
        vector, near_cols, near_blocks, col_basis, row_basis, leaf_far, leaf_coupling,
        leaf_transfer, box_far, box_coupling, box_transfer, coarse_far, coarse_coupling,
    )}

    def placed(arrays):
        return [
            pltpu.with_memory_space_constraint(a, pltpu.HBM if id(a) in given else pltpu.VMEM)
            for a in arrays
        ]

    def made(*dims, dtype=F32):
        return pltpu.VMEM(dims, dtype)

    def call(kernel, inputs, outs, smem=(), hbm=(), scratch=()):
        specs = [SMEM] * len(smem) + [VMEM] * len(inputs)
        specs += [pl.BlockSpec(memory_space=pl.ANY)] * len(hbm)
        return pl.pallas_call(
            kernel,
            in_specs=specs,
            out_specs=[VMEM] * len(outs),
            out_shape=outs,
            scratch_shapes=scratch,
            compiler_params=params,
        )(*placed(smem), *placed(inputs), *placed(hbm))

    half = group // 2
    across = []
    for i in range(rows - 1):
        for j in range(half):
            pair = (i * group + group - 1 - j, (i + 1) * group + j)
            across += [pair, pair[::-1]]
    inside = [(i, i ^ half) for i in range(devices)]

    def exchange(packet, number):
        own = lax.all_to_all(packet, GRP, 0, 0, tiled=True)
        mine, parent = call(
            group_kernel, [own], [made(side, lanes, dtype=BF), made(rows, dense, lanes, dtype=BF)]
        )
        near_side = lax.ppermute(mine, ROWS_GRP, across)
        parents = lax.all_to_all(parent, ROWS, 0, 0, tiled=True)
        far_side = lax.ppermute(near_side, ROWS_GRP, inside)
        (near,) = call(
            near_kernel,
            [own, near_side],
            [made(flat, width)],
            smem=[near_cols],
            hbm=[near_blocks],
            scratch=[
                pltpu.VMEM((group + 2, leaves * tiles * nrhs, lanes), BF),
                pltpu.VMEM((leaves, kn, width, width), BF),
                pltpu.SemaphoreType.DMA((leaves,)),
            ],
        )
        inputs = [own, near_side, far_side, leaf_coupling, box_coupling, leaf_transfer]
        outs = [made(flat, lanes)]
        kernel = fine_kernel
        if number == 0:
            kernel = fine_and_stage_kernel
            inputs += [coarse_coupling, box_transfer, row_basis, col_basis, vector]
            outs += [
                made(R, lanes, dtype=BF), made(lanes, R, dtype=BF),
                made(lanes, width, dtype=BF), made(lanes, width, dtype=BF),
                made(lanes, R, dtype=BF), made(R, R, dtype=BF), made(*vector.shape),
            ]
        local_field, *staged = call(
            kernel,
            inputs,
            outs,
            smem=[leaf_far, box_far],
            scratch=[pltpu.VMEM((3 * group, 2 * nrhs, lanes), BF)],
        )
        return [parents, near, local_field], staged

    packet_out = made(group, size, lanes, dtype=BF)
    stack = pltpu.VMEM((coarse_far.shape[1] * dense, lanes), F32)
    (packet,) = call(start_kernel, [vector, col_basis, leaf_transfer, box_transfer], [packet_out])
    received, staged = exchange(packet, 0)
    coarse, down, row_flat, col_flat, leaf_up, box_up, first = staged
    image, packet = call(
        middle_kernel,
        received + [coarse, down, row_flat, col_flat, leaf_up, box_up],
        [made(flat, width), packet_out],
        smem=[coarse_far],
        scratch=[stack],
    )
    received, _ = exchange(packet, 1)
    second, sums = call(
        products_kernel,
        received + [coarse, down, row_flat, first, image],
        [made(flat, width), made(devices, 1, 8 * nrhs)],
        smem=[coarse_far],
        scratch=[stack],
    )
    sums = lax.all_to_all(sums, ROWS_GRP, 0, 0, tiled=True)
    shape = jax.ShapeDtypeStruct
    basis, remainder, hessenberg = call(
        finish_kernel,
        [sums, first, image, second],
        [shape(vector.shape, F32), shape(vector.shape, F32), shape((5, nrhs), F32)],
    )
    return basis, remainder, hessenberg.T


def solution(mesh):
    finer = Mesh(
        mesh.devices.reshape(4, 4, 4, 2, 2), ("rows_0", "rows_1", "rows_2", "grp_0", "grp_1")
    )
    placed = (
        P(ROWS_GRP, None, None),
        P(ROWS_GRP, None),
        P(ROWS_GRP, None, None, None),
        P(ROWS_GRP, None, None),
        P(ROWS_GRP, None, None),
        P(ROWS_GRP, None),
        P(ROWS_GRP, None, None),
        P(ROWS_GRP, None, None),
        P(ROWS_GRP, None),
        P(ROWS_GRP, None, None),
        P(ROWS_GRP, None, None),
        P(ROWS, None),
        P(ROWS, None, None),
    )
    return jax.shard_map(
        shards,
        mesh=finer,
        in_specs=placed,
        out_specs=(P(ROWS_GRP, None, None), P(ROWS_GRP, None, None), P()),
        check_vma=False,
    )
```

```python
import jax
import jax.numpy as jnp
from jax import lax
from jax.experimental import pallas as pl
from jax.experimental.pallas import tpu as pltpu
from jax.sharding import Mesh
from jax.sharding import PartitionSpec as P


R = 32
GRP = ("grp_0", "grp_1")
ROWS = ("rows_0", "rows_1", "rows_2")
ROWS_GRP = ("rows_0", "rows_1", "rows_2", "grp_0", "grp_1")
BF = jnp.bfloat16
F32 = jnp.float32

epsilon = 1e-06
SMALL = 2.0**-40
SWITCH = 2.0**-20
LIMIT = 16 * 2**20

NT = (((1,), (1,)), ((), ()))
NN = (((1,), (0,)), ((), ()))

VMEM = pl.BlockSpec(memory_space=pltpu.VMEM)
SMEM = pl.BlockSpec(memory_space=pltpu.SMEM)


def dot(left, right, dims=NN):
    return lax.dot_general(left, right, dims, preferred_element_type=F32)


def row_col(shape):
    return (
        lax.broadcasted_iota(jnp.int32, shape, 0),
        lax.broadcasted_iota(jnp.int32, shape, 1),
    )


def diagonal(leaves, nrhs):
    row, col = row_col((leaves * nrhs, leaves * R))
    return row // nrhs == col // R


def over_leaves(array, leaves):
    step = array.shape[0] // leaves
    total = array[:step]
    for l in range(1, leaves):
        total = total + array[l * step : (l + 1) * step]
    return total


def coefficients(field_bf, col_basis, leaf_transfer, box_transfer, packet_ref, coef_ref):
    lanes = col_basis.shape[0]
    leaves = lanes // R
    nrhs = field_bf.shape[0] // leaves
    full = dot(field_bf, col_basis, NT)
    leaf = over_leaves(jnp.where(diagonal(leaves, nrhs), full, 0.0), leaves).astype(BF)
    box = dot(leaf, leaf_transfer).astype(BF)
    parent = dot(box, box_transfer).astype(BF)
    row, col = row_col((R, lanes))
    both = dot(box, (row == col).astype(BF)) + dot(parent, (row + R == col).astype(BF))
    blocks = []
    for l in range(leaves):
        for t in range(field_bf.shape[1] // lanes):
            blocks.append(field_bf[l * nrhs : (l + 1) * nrhs, t * lanes : (t + 1) * lanes])
    coef = [leaf, both.astype(BF)]
    packet_ref[...] = jnp.concatenate(blocks + coef, axis=0)
    coef_ref[...] = jnp.concatenate(coef, axis=0)


def start_kernel(vector, col_basis, leaf_transfer, box_transfer, packet_ref, coef_ref):
    leaves, nrhs, width = vector.shape
    field = vector[...].reshape(leaves * nrhs, width).astype(BF)
    coefficients(
        field,
        col_basis[...].reshape(leaves * R, width),
        leaf_transfer[...].reshape(leaves * R, R).astype(BF),
        box_transfer[0].astype(BF),
        packet_ref,
        coef_ref,
    )


def group_kernel(own, chip, cross, coef, side_ref, parent_ref):
    size, lanes = own.shape
    nrhs = coef.shape[0] // 2
    fields = size - 2 * nrhs
    place = position()
    side_ref[:fields] = own[:fields]
    total = None
    for other, part in ((0, own[fields:]), (1, chip[fields:]), (3, cross[fields:]), (2, coef[...])):
        first = pl.multiple_of(fields + (place ^ other) * (2 * nrhs), 2 * nrhs)
        side_ref[pl.ds(first, 2 * nrhs)] = part
        parent = part[nrhs:].astype(F32)
        total = parent if total is None else total + parent
    total = total.astype(BF)
    row, col = row_col((lanes, lanes))
    tiled = dot(total, ((row // R == 1) & (row % R == col % R)).astype(BF))
    per_row = parent_ref.shape[1]
    row, col = row_col((nrhs, lanes))
    tiled = jnp.where(row // per_row == col // R, tiled, 0.0).astype(BF)
    row, col = row_col((8, nrhs))
    dense = dot((row == col % per_row).astype(BF), tiled).astype(BF)[:per_row]
    parent_ref[...] = jnp.broadcast_to(dense[None], parent_ref.shape)


def position():
    return lax.axis_index(GRP[0]) * lax.axis_size(GRP[1]) + lax.axis_index(GRP[1])


def row_index():
    index = lax.axis_index(ROWS[0])
    for axis in ROWS[1:]:
        index = index * lax.axis_size(axis) + lax.axis_index(axis)
    return index


def near_kernel(near_cols, own, chip, cross, side, blocks, out, window, weights, sems):
    leaves, kn, _, _ = blocks.shape
    nrhs = out.shape[0] // leaves
    group = window.shape[0] - 2
    fields = window.shape[1]
    copies = [
        pltpu.make_async_copy(blocks.at[l], weights.at[l], sems.at[l]) for l in range(leaves)
    ]
    for copy in copies:
        copy.start()
    window[0] = side[:fields]
    window[group + 1] = side[:fields]
    place = position()
    window[place + 1] = own[:fields]
    window[(place ^ 1) + 1] = chip[:fields]
    window[(place ^ 3) + 1] = cross[:fields]
    base = (row_index() * group - 1) * leaves
    tiles = fields // leaves // nrhs
    for l in range(leaves):
        picked = []
        for k in range(kn):
            index = near_cols[l, k] - base
            device = index // leaves
            first = (index - device * leaves) * (tiles * nrhs)
            picked += [
                window[device, pl.ds(pl.multiple_of(first + t * nrhs, nrhs), nrhs)]
                for t in range(tiles)
            ]
        copies[l].wait()
        total = None
        for k in range(kn):
            part = jnp.concatenate(picked[k * tiles : (k + 1) * tiles], axis=1)
            term = dot(part, weights[l, k], NT)
            total = term if total is None else total + term
        out[l * nrhs : (l + 1) * nrhs] = total


def fine_sums(
    leaf_far, box_far, own, side, other, leaf_coupling, box_coupling, leaf_transfer, out, window
):
    size, lanes = own.shape
    leaves, kf = leaf_far.shape
    nrhs = out.shape[0] // leaves
    group = window.shape[0] // 3
    fields = size - 2 * group * nrhs
    is_low = position() < group // 2
    side_slot = jnp.where(is_low, 0, 2 * group)
    other_slot = jnp.where(is_low, 2 * group, 0)
    for j in range(group):
        rows = slice(fields + j * 2 * nrhs, fields + (j + 1) * 2 * nrhs)
        window[side_slot + j] = side[rows]
        window[group + j] = own[rows]
        window[other_slot + j] = other[rows]
    first_box = (row_index() - 1) * group
    first_leaf = first_box * leaves
    _, col = row_col((nrhs, lanes))
    block = col // R
    per_tile = lanes // R
    rows = []
    for l in range(leaves):
        tiles = []
        for t in range(kf // per_tile):
            tile = jnp.zeros((nrhs, lanes), F32)
            for i in range(per_tile):
                index = leaf_far[l, t * per_tile + i] - first_leaf
                box = index // leaves
                item = index - box * leaves
                values = window[box, :nrhs].astype(F32)
                shift = lax.rem(i - item + per_tile, per_tile) * R
                values = pltpu.roll(values, shift, 1)
                tile = jnp.where(block == i, values, tile)
            tiles.append(tile.astype(BF))
        rows.append(jnp.concatenate(tiles, axis=1))
    gathered = jnp.concatenate(rows, axis=0)
    leaf_field = dot(gathered, leaf_coupling[...].reshape(leaves * R, -1), NT)
    tile = jnp.zeros((nrhs, lanes), F32)
    for k in range(box_far.shape[1]):
        values = window[box_far[0, k] - first_box, nrhs:].astype(F32)
        if k:
            values = pltpu.roll(values, k * R, 1)
        tile = jnp.where(block == k, values, tile)
    box_field = dot(tile.astype(BF), box_coupling[0], NT)
    transfer = leaf_transfer[...].reshape(leaves * R, R)
    shared = lax.dot_general(
        box_field, transfer, NT, precision=lax.Precision.HIGHEST, preferred_element_type=F32
    )
    out[...] = leaf_field + jnp.concatenate([shared] * leaves, axis=0)


def fine_kernel(
    leaf_far, box_far, own, side, other, leaf_coupling, box_coupling, leaf_transfer, out, window
):
    fine_sums(
        leaf_far, box_far, own, side, other, leaf_coupling, box_coupling, leaf_transfer, out,
        window,
    )


def fine_and_stage_kernel(
    leaf_far, box_far, own, side, other, leaf_coupling, box_coupling, leaf_transfer,
    coarse_coupling, box_transfer, row_basis, col_basis, vector, out, coarse_out, down_out,
    row_out, col_out, leaf_out, box_out, vector_out, window,
):
    fine_sums(
        leaf_far, box_far, own, side, other, leaf_coupling, box_coupling, leaf_transfer, out,
        window,
    )
    transfer = leaf_transfer[...].reshape(leaf_out.shape)
    coarse_out[...] = coarse_coupling[0]
    down_out[...] = lax.dot_general(
        transfer, box_transfer[0], NN, precision=lax.Precision.HIGHEST,
        preferred_element_type=F32,
    ).astype(BF)
    row_out[...] = row_basis[...].reshape(row_out.shape)
    col_out[...] = col_basis[...].reshape(col_out.shape)
    leaf_out[...] = transfer.astype(BF)
    box_out[...] = box_transfer[0].astype(BF)
    vector_out[...] = vector[...]


def downward(coarse_far, parents, near, local_field, coarse_coupling, down, row_basis, stack):
    kc = coarse_far.shape[1]
    per_row, lanes = parents.shape[1:]
    leaves = lanes // R
    nrhs = near.shape[0] // leaves
    for k in range(kc):
        stack[k * per_row : (k + 1) * per_row] = parents[coarse_far[0, k]].astype(F32)
    dense = stack[...].astype(BF)
    row, col = row_col((kc * nrhs, kc * per_row))
    pick = (row // nrhs == col // per_row) & (row % per_row == col % per_row)
    wide = dot(pick.astype(BF), dense)
    row, col = row_col((kc * nrhs, lanes))
    wide = jnp.where(row % nrhs // per_row == col // R, wide, 0.0)
    half = wide + pltpu.roll(wide, 2 * R, 1)
    wide = half + pltpu.roll(half, R, 1)
    wide = jnp.where(row // nrhs == col // R, wide, 0.0)
    gathered = over_leaves(wide, kc).astype(BF)
    group_field = dot(gathered, coarse_coupling[...], NT)
    shared = dot(group_field.astype(BF), down[...], NT)
    local = local_field[...] + jnp.concatenate([shared] * leaves, axis=0)
    local = jnp.where(diagonal(leaves, nrhs), local, 0.0).astype(BF)
    return near[...] + dot(local, row_basis[...])


def middle_kernel(
    coarse_far, parents, near, local_field, coarse_coupling, down, row_basis, col_basis,
    leaf_transfer, box_transfer, image_ref, packet_ref, coef_ref, stack,
):
    image = downward(
        coarse_far, parents, near, local_field, coarse_coupling, down, row_basis, stack
    )
    image_ref[...] = image
    coefficients(
        image.astype(BF), col_basis[...], leaf_transfer[...], box_transfer[...], packet_ref,
        coef_ref,
    )


def products_kernel(
    coarse_far, parents, near, local_field, coarse_coupling, down, row_basis, vector, image,
    second_ref, sums_ref, stack,
):
    leaves, nrhs, width = vector.shape
    second = downward(
        coarse_far, parents, near, local_field, coarse_coupling, down, row_basis, stack
    )
    second_ref[...] = second
    first = vector[...].reshape(leaves * nrhs, width)
    middle = image[...]
    small = second * SMALL
    pairs = (
        (first, first), (first, middle), (middle, middle), (first, second),
        (middle, second), (second, second), (middle, small), (small, small),
    )
    parts = []
    for left, right in pairs:
        product = over_leaves(left * right, leaves)
        part = product[:, :128]
        for i in range(1, width // 128):
            part = part + product[:, i * 128 : (i + 1) * 128]
        parts.append(part)
    table = jnp.concatenate(parts, axis=0)
    sums = jnp.sum(table.T, axis=0, keepdims=True)
    sums_ref[...] = jnp.broadcast_to(sums[None], sums_ref.shape)


def finish_kernel(sums, vector, image, second, basis_ref, remainder_ref, hessenberg_ref):
    leaves, nrhs, width = vector.shape
    count = sums.shape[0] * leaves * width
    total = jnp.sum(sums[...], axis=0)
    row, col = row_col((nrhs, total.shape[1]))
    total = jnp.broadcast_to(total, (nrhs, total.shape[1]))

    def mean(i):
        own = jnp.where(col == i * nrhs + row, total, 0.0)
        return jnp.sum(own, axis=1, keepdims=True) / count

    vv, vu, uu, vz = mean(0), mean(1), mean(2), mean(3)
    large = mean(7) > SWITCH
    uz = jnp.where(large, mean(6), mean(4))
    zz = jnp.where(large, mean(7), mean(5))
    unit = jnp.where(large, 1.0 / SMALL, 1.0)
    square_first = vv + epsilon
    norm_first = jnp.sqrt(square_first)
    ratio = vu / square_first
    proj_first = 0.5 * vv / square_first + ratio
    shift = proj_first - 0.5
    square_image = (uu - 2.0 * shift * vu + shift * shift * vv) / square_first
    norm_image = jnp.sqrt(square_image + epsilon)
    scale = 1.0 / (norm_first * norm_image)
    on_z = scale * unit
    on_u = scale * (0.5 - shift)
    on_v = -0.5 * shift * scale
    v_with = scale * vz + on_u * vu + on_v * vv
    u_with = on_z * uz + on_u * uu + on_v * vu
    proj_second = v_with / norm_first
    cross = scale * (vu - shift * vv) / norm_first
    proj_basis = scale * u_with - scale * shift * v_with - proj_second * cross
    on_u = on_u - proj_basis * scale
    on_v = on_v - proj_second / norm_first + proj_basis * scale * shift
    square_last = (
        on_z * (on_z * zz)
        + 2.0 * on_u * (on_z * uz)
        + 2.0 * on_v * (scale * vz)
        + on_u * (on_u * uu)
        + 2.0 * on_v * (on_u * vu)
        + on_v * (on_v * vv)
    )
    norm_last = jnp.sqrt(square_last + epsilon)
    for l in range(leaves):
        rows = pl.ds(l * nrhs, nrhs)
        v = vector[l]
        u = image[rows, :]
        basis_ref[l] = scale * u - (scale * shift) * v
        remainder_ref[l] = scale * second[rows, :] + on_u * u + on_v * v
    entries = (proj_first, norm_image, proj_second, proj_basis, norm_last)
    row, col = row_col((nrhs, nrhs))
    for i, entry in enumerate(entries):
        line = jnp.sum(jnp.where(row == col, entry, 0.0), axis=0, keepdims=True)
        hessenberg_ref[i : i + 1] = line


def shards(
    vector,
    near_cols,
    near_blocks,
    col_basis,
    row_basis,
    leaf_far,
    leaf_coupling,
    leaf_transfer,
    box_far,
    box_coupling,
    box_transfer,
    coarse_far,
    coarse_coupling,
):
    leaves, nrhs, width = vector.shape
    group = lax.axis_size(GRP)
    rows = lax.axis_size(ROWS)
    devices = rows * group
    kn = near_cols.shape[1]
    lanes = leaves * R
    flat = leaves * nrhs
    dense = nrhs * R // lanes
    tiles = width // lanes
    size = (leaves * tiles + 2) * nrhs
    side = (leaves * tiles + 2 * group) * nrhs
    params = pltpu.CompilerParams(vmem_limit_bytes=LIMIT)

    given = {id(a) for a in (
        vector, near_cols, near_blocks, col_basis, row_basis, leaf_far, leaf_coupling,
        leaf_transfer, box_far, box_coupling, box_transfer, coarse_far, coarse_coupling,
    )}

    def placed(arrays):
        return [
            pltpu.with_memory_space_constraint(a, pltpu.HBM if id(a) in given else pltpu.VMEM)
            for a in arrays
        ]

    def made(*dims, dtype=F32):
        return pltpu.VMEM(dims, dtype)

    def call(kernel, inputs, outs, smem=(), hbm=(), scratch=()):
        specs = [SMEM] * len(smem) + [VMEM] * len(inputs)
        specs += [pl.BlockSpec(memory_space=pl.ANY)] * len(hbm)
        return pl.pallas_call(
            kernel,
            in_specs=specs,
            out_specs=[VMEM] * len(outs),
            out_shape=outs,
            scratch_shapes=scratch,
            compiler_params=params,
        )(*placed(smem), *placed(inputs), *placed(hbm))

    half = group // 2
    across = []
    for i in range(rows - 1):
        for j in range(half):
            pair = (i * group + group - 1 - j, (i + 1) * group + j)
            across += [pair, pair[::-1]]

    def swap(array, bits):
        return lax.ppermute(array, ROWS_GRP, [(i, i ^ bits) for i in range(devices)])

    def exchange(packet, coef, number):
        chip = swap(packet, 1)
        cross = swap(packet, 3)
        third = swap(coef, 2)
        mine, parent = call(
            group_kernel,
            [packet, chip, cross, third],
            [made(side, lanes, dtype=BF), made(rows, dense, lanes, dtype=BF)],
        )
        near_side = lax.ppermute(mine, ROWS_GRP, across)
        parents = lax.all_to_all(parent, ROWS, 0, 0, tiled=True)
        far_side = swap(near_side, half)
        (near,) = call(
            near_kernel,
            [packet, chip, cross, near_side],
            [made(flat, width)],
            smem=[near_cols],
            hbm=[near_blocks],
            scratch=[
                pltpu.VMEM((group + 2, leaves * tiles * nrhs, lanes), BF),
                pltpu.VMEM((leaves, kn, width, width), BF),
                pltpu.SemaphoreType.DMA((leaves,)),
            ],
        )
        inputs = [mine, near_side, far_side, leaf_coupling, box_coupling, leaf_transfer]
        outs = [made(flat, lanes)]
        kernel = fine_kernel
        if number == 0:
            kernel = fine_and_stage_kernel
            inputs += [coarse_coupling, box_transfer, row_basis, col_basis, vector]
            outs += [
                made(R, lanes, dtype=BF), made(lanes, R, dtype=BF),
                made(lanes, width, dtype=BF), made(lanes, width, dtype=BF),
                made(lanes, R, dtype=BF), made(R, R, dtype=BF), made(*vector.shape),
            ]
        local_field, *staged = call(
            kernel,
            inputs,
            outs,
            smem=[leaf_far, box_far],
            scratch=[pltpu.VMEM((3 * group, 2 * nrhs, lanes), BF)],
        )
        return [parents, near, local_field], staged

    upward_out = [made(size, lanes, dtype=BF), made(2 * nrhs, lanes, dtype=BF)]
    stack = pltpu.VMEM((coarse_far.shape[1] * dense, lanes), F32)
    upward = call(start_kernel, [vector, col_basis, leaf_transfer, box_transfer], upward_out)
    received, staged = exchange(*upward, 0)
    coarse, down, row_flat, col_flat, leaf_up, box_up, first = staged
    image, *upward = call(
        middle_kernel,
        received + [coarse, down, row_flat, col_flat, leaf_up, box_up],
        [made(flat, width), *upward_out],
        smem=[coarse_far],
        scratch=[stack],
    )
    received, _ = exchange(*upward, 1)
    second, sums = call(
        products_kernel,
        received + [coarse, down, row_flat, first, image],
        [made(flat, width), made(devices, 1, 8 * nrhs)],
        smem=[coarse_far],
        scratch=[stack],
    )
    sums = lax.all_to_all(sums, ROWS_GRP, 0, 0, tiled=True)
    shape = jax.ShapeDtypeStruct
    basis, remainder, hessenberg = call(
        finish_kernel,
        [sums, first, image, second],
        [shape(vector.shape, F32), shape(vector.shape, F32), shape((5, nrhs), F32)],
    )
    return basis, remainder, hessenberg.T


def solution(mesh):
    finer = Mesh(
        mesh.devices.reshape(4, 4, 4, 2, 2), ("rows_0", "rows_1", "rows_2", "grp_0", "grp_1")
    )
    placed = (
        P(ROWS_GRP, None, None),
        P(ROWS_GRP, None),
        P(ROWS_GRP, None, None, None),
        P(ROWS_GRP, None, None),
        P(ROWS_GRP, None, None),
        P(ROWS_GRP, None),
        P(ROWS_GRP, None, None),
        P(ROWS_GRP, None, None),
        P(ROWS_GRP, None),
        P(ROWS_GRP, None, None),
        P(ROWS_GRP, None, None),
        P(ROWS, None),
        P(ROWS, None, None),
    )
    return jax.shard_map(
        shards,
        mesh=finer,
        in_specs=placed,
        out_specs=(P(ROWS_GRP, None, None), P(ROWS_GRP, None, None), P()),
        check_vma=False,
    )
```

```python
import jax
import jax.numpy as jnp
from jax import lax
from jax.experimental import pallas as pl
from jax.experimental.pallas import tpu as pltpu
from jax.sharding import Mesh
from jax.sharding import PartitionSpec as P


R = 32
GRP = ("grp_0", "grp_1")
ROWS = ("rows_0", "rows_1", "rows_2")
ROWS_GRP = ("rows_0", "rows_1", "rows_2", "grp_0", "grp_1")
BF = jnp.bfloat16
F32 = jnp.float32

epsilon = 1e-06
SMALL = 2.0**-40
SWITCH = 2.0**-20
LIMIT = 16 * 2**20

NT = (((1,), (1,)), ((), ()))
NN = (((1,), (0,)), ((), ()))

VMEM = pl.BlockSpec(memory_space=pltpu.VMEM)
SMEM = pl.BlockSpec(memory_space=pltpu.SMEM)


def dot(left, right, dims=NN):
    return lax.dot_general(left, right, dims, preferred_element_type=F32)


def row_col(shape):
    return (
        lax.broadcasted_iota(jnp.int32, shape, 0),
        lax.broadcasted_iota(jnp.int32, shape, 1),
    )


def diagonal(leaves, nrhs):
    row, col = row_col((leaves * nrhs, leaves * R))
    return row // nrhs == col // R


def over_leaves(array, leaves):
    step = array.shape[0] // leaves
    total = array[:step]
    for l in range(1, leaves):
        total = total + array[l * step : (l + 1) * step]
    return total


def coefficients(field_bf, col_basis, leaf_transfer, box_transfer, tiles_ref, coef_ref):
    lanes = col_basis.shape[0]
    leaves = lanes // R
    nrhs = field_bf.shape[0] // leaves
    full = dot(field_bf, col_basis, NT)
    leaf = over_leaves(jnp.where(diagonal(leaves, nrhs), full, 0.0), leaves).astype(BF)
    box = dot(leaf, leaf_transfer).astype(BF)
    parent = dot(box, box_transfer).astype(BF)
    row, col = row_col((R, lanes))
    both = dot(box, (row == col).astype(BF)) + dot(parent, (row + R == col).astype(BF))
    blocks = []
    for l in range(leaves):
        for t in range(field_bf.shape[1] // lanes):
            blocks.append(field_bf[l * nrhs : (l + 1) * nrhs, t * lanes : (t + 1) * lanes])
    coef = [leaf, both.astype(BF)]
    tiles_ref[...] = jnp.concatenate(blocks, axis=0)
    coef_ref[...] = jnp.concatenate(coef, axis=0)


def start_kernel(vector, col_basis, leaf_transfer, box_transfer, tiles_ref, coef_ref):
    leaves, nrhs, width = vector.shape
    field = vector[...].reshape(leaves * nrhs, width).astype(BF)
    coefficients(
        field,
        col_basis[...].reshape(leaves * R, width),
        leaf_transfer[...].reshape(leaves * R, R).astype(BF),
        box_transfer[0].astype(BF),
        tiles_ref,
        coef_ref,
    )


def group_kernel(tiles, coef, chip, cross, third, side_ref, parent_ref):
    fields, lanes = tiles.shape
    nrhs = coef.shape[0] // 2
    place = position()
    side_ref[:fields] = tiles[...]
    total = None
    for other, source in ((0, coef), (1, chip), (3, cross), (2, third)):
        part = source[...]
        first = pl.multiple_of(fields + (place ^ other) * (2 * nrhs), 2 * nrhs)
        side_ref[pl.ds(first, 2 * nrhs)] = part
        parent = part[nrhs:].astype(F32)
        total = parent if total is None else total + parent
    total = total.astype(BF)
    row, col = row_col((lanes, lanes))
    tiled = dot(total, ((row // R == 1) & (row % R == col % R)).astype(BF))
    per_row = parent_ref.shape[1]
    row, col = row_col((nrhs, lanes))
    tiled = jnp.where(row // per_row == col // R, tiled, 0.0).astype(BF)
    row, col = row_col((8, nrhs))
    dense = dot((row == col % per_row).astype(BF), tiled).astype(BF)[:per_row]
    parent_ref[...] = jnp.broadcast_to(dense[None], parent_ref.shape)


def position():
    return lax.axis_index(GRP[0]) * lax.axis_size(GRP[1]) + lax.axis_index(GRP[1])


def row_index():
    index = lax.axis_index(ROWS[0])
    for axis in ROWS[1:]:
        index = index * lax.axis_size(axis) + lax.axis_index(axis)
    return index


def near_kernel(near_cols, own, chip, cross, side, blocks, out, window, weights, sems):
    leaves, kn, _, _ = blocks.shape
    nrhs = out.shape[0] // leaves
    group = window.shape[0] - 2
    fields = window.shape[1]
    copies = [
        pltpu.make_async_copy(blocks.at[l], weights.at[l], sems.at[l]) for l in range(leaves)
    ]
    for copy in copies:
        copy.start()
    window[0] = side[:fields]
    window[group + 1] = side[:fields]
    place = position()
    window[place + 1] = own[...]
    window[(place ^ 1) + 1] = chip[...]
    window[(place ^ 3) + 1] = cross[...]
    base = (row_index() * group - 1) * leaves
    tiles = fields // leaves // nrhs
    for l in range(leaves):
        picked = []
        for k in range(kn):
            index = near_cols[l, k] - base
            device = index // leaves
            first = (index - device * leaves) * (tiles * nrhs)
            picked += [
                window[device, pl.ds(pl.multiple_of(first + t * nrhs, nrhs), nrhs)]
                for t in range(tiles)
            ]
        copies[l].wait()
        total = None
        for k in range(kn):
            part = jnp.concatenate(picked[k * tiles : (k + 1) * tiles], axis=1)
            term = dot(part, weights[l, k], NT)
            total = term if total is None else total + term
        out[l * nrhs : (l + 1) * nrhs] = total


def fine_sums(
    leaf_far, box_far, own, side, other, leaf_coupling, box_coupling, leaf_transfer, out, window
):
    size, lanes = own.shape
    leaves, kf = leaf_far.shape
    nrhs = out.shape[0] // leaves
    group = window.shape[0] // 3
    fields = size - 2 * group * nrhs
    is_low = position() < group // 2
    side_slot = jnp.where(is_low, 0, 2 * group)
    other_slot = jnp.where(is_low, 2 * group, 0)
    for j in range(group):
        rows = slice(fields + j * 2 * nrhs, fields + (j + 1) * 2 * nrhs)
        window[side_slot + j] = side[rows]
        window[group + j] = own[rows]
        window[other_slot + j] = other[rows]
    first_box = (row_index() - 1) * group
    first_leaf = first_box * leaves
    _, col = row_col((nrhs, lanes))
    block = col // R
    per_tile = lanes // R
    rows = []
    for l in range(leaves):
        tiles = []
        for t in range(kf // per_tile):
            tile = jnp.zeros((nrhs, lanes), F32)
            for i in range(per_tile):
                index = leaf_far[l, t * per_tile + i] - first_leaf
                box = index // leaves
                item = index - box * leaves
                values = window[box, :nrhs].astype(F32)
                shift = lax.rem(i - item + per_tile, per_tile) * R
                values = pltpu.roll(values, shift, 1)
                tile = jnp.where(block == i, values, tile)
            tiles.append(tile.astype(BF))
        rows.append(jnp.concatenate(tiles, axis=1))
    gathered = jnp.concatenate(rows, axis=0)
    leaf_field = dot(gathered, leaf_coupling[...].reshape(leaves * R, -1), NT)
    tile = jnp.zeros((nrhs, lanes), F32)
    for k in range(box_far.shape[1]):
        values = window[box_far[0, k] - first_box, nrhs:].astype(F32)
        if k:
            values = pltpu.roll(values, k * R, 1)
        tile = jnp.where(block == k, values, tile)
    box_field = dot(tile.astype(BF), box_coupling[0], NT)
    transfer = leaf_transfer[...].reshape(leaves * R, R)
    shared = lax.dot_general(
        box_field, transfer, NT, precision=lax.Precision.HIGHEST, preferred_element_type=F32
    )
    out[...] = leaf_field + jnp.concatenate([shared] * leaves, axis=0)


def fine_kernel(
    leaf_far, box_far, own, side, other, leaf_coupling, box_coupling, leaf_transfer, out, window
):
    fine_sums(
        leaf_far, box_far, own, side, other, leaf_coupling, box_coupling, leaf_transfer, out,
        window,
    )


def fine_and_stage_kernel(
    leaf_far, box_far, own, side, other, leaf_coupling, box_coupling, leaf_transfer,
    coarse_coupling, box_transfer, row_basis, col_basis, vector, out, coarse_out, down_out,
    row_out, col_out, leaf_out, box_out, vector_out, window,
):
    fine_sums(
        leaf_far, box_far, own, side, other, leaf_coupling, box_coupling, leaf_transfer, out,
        window,
    )
    transfer = leaf_transfer[...].reshape(leaf_out.shape)
    coarse_out[...] = coarse_coupling[0]
    down_out[...] = lax.dot_general(
        transfer, box_transfer[0], NN, precision=lax.Precision.HIGHEST,
        preferred_element_type=F32,
    ).astype(BF)
    row_out[...] = row_basis[...].reshape(row_out.shape)
    col_out[...] = col_basis[...].reshape(col_out.shape)
    leaf_out[...] = transfer.astype(BF)
    box_out[...] = box_transfer[0].astype(BF)
    vector_out[...] = vector[...]


def downward(coarse_far, parents, near, local_field, coarse_coupling, down, row_basis, stack):
    kc = coarse_far.shape[1]
    per_row, lanes = parents.shape[1:]
    leaves = lanes // R
    nrhs = near.shape[0] // leaves
    for k in range(kc):
        stack[k * per_row : (k + 1) * per_row] = parents[coarse_far[0, k]].astype(F32)
    dense = stack[...].astype(BF)
    row, col = row_col((kc * nrhs, kc * per_row))
    pick = (row // nrhs == col // per_row) & (row % per_row == col % per_row)
    wide = dot(pick.astype(BF), dense)
    row, col = row_col((kc * nrhs, lanes))
    wide = jnp.where(row % nrhs // per_row == col // R, wide, 0.0)
    half = wide + pltpu.roll(wide, 2 * R, 1)
    wide = half + pltpu.roll(half, R, 1)
    wide = jnp.where(row // nrhs == col // R, wide, 0.0)
    gathered = over_leaves(wide, kc).astype(BF)
    group_field = dot(gathered, coarse_coupling[...], NT)
    shared = dot(group_field.astype(BF), down[...], NT)
    local = local_field[...] + jnp.concatenate([shared] * leaves, axis=0)
    local = jnp.where(diagonal(leaves, nrhs), local, 0.0).astype(BF)
    return near[...] + dot(local, row_basis[...])


def middle_kernel(
    coarse_far, parents, near, local_field, coarse_coupling, down, row_basis, col_basis,
    leaf_transfer, box_transfer, image_ref, tiles_ref, coef_ref, stack,
):
    image = downward(
        coarse_far, parents, near, local_field, coarse_coupling, down, row_basis, stack
    )
    image_ref[...] = image
    coefficients(
        image.astype(BF), col_basis[...], leaf_transfer[...], box_transfer[...], tiles_ref,
        coef_ref,
    )


def products_kernel(
    coarse_far, parents, near, local_field, coarse_coupling, down, row_basis, vector, image,
    second_ref, sums_ref, stack,
):
    leaves, nrhs, width = vector.shape
    second = downward(
        coarse_far, parents, near, local_field, coarse_coupling, down, row_basis, stack
    )
    second_ref[...] = second
    first = vector[...].reshape(leaves * nrhs, width)
    middle = image[...]
    small = second * SMALL
    pairs = (
        (first, first), (first, middle), (middle, middle), (first, second),
        (middle, second), (second, second), (middle, small), (small, small),
    )
    parts = []
    for left, right in pairs:
        product = over_leaves(left * right, leaves)
        part = product[:, :128]
        for i in range(1, width // 128):
            part = part + product[:, i * 128 : (i + 1) * 128]
        parts.append(part)
    table = jnp.concatenate(parts, axis=0)
    sums = jnp.sum(table.T, axis=0, keepdims=True)
    sums_ref[...] = jnp.broadcast_to(sums[None], sums_ref.shape)


def finish_kernel(sums, vector, image, second, basis_ref, remainder_ref, hessenberg_ref):
    leaves, nrhs, width = vector.shape
    count = sums.shape[0] * leaves * width
    total = jnp.sum(sums[...], axis=0)
    row, col = row_col((nrhs, total.shape[1]))
    total = jnp.broadcast_to(total, (nrhs, total.shape[1]))

    def mean(i):
        own = jnp.where(col == i * nrhs + row, total, 0.0)
        return jnp.sum(own, axis=1, keepdims=True) / count

    vv, vu, uu, vz = mean(0), mean(1), mean(2), mean(3)
    large = mean(7) > SWITCH
    uz = jnp.where(large, mean(6), mean(4))
    zz = jnp.where(large, mean(7), mean(5))
    unit = jnp.where(large, 1.0 / SMALL, 1.0)
    square_first = vv + epsilon
    norm_first = jnp.sqrt(square_first)
    ratio = vu / square_first
    proj_first = 0.5 * vv / square_first + ratio
    shift = proj_first - 0.5
    square_image = (uu - 2.0 * shift * vu + shift * shift * vv) / square_first
    norm_image = jnp.sqrt(square_image + epsilon)
    scale = 1.0 / (norm_first * norm_image)
    on_z = scale * unit
    on_u = scale * (0.5 - shift)
    on_v = -0.5 * shift * scale
    v_with = scale * vz + on_u * vu + on_v * vv
    u_with = on_z * uz + on_u * uu + on_v * vu
    proj_second = v_with / norm_first
    cross = scale * (vu - shift * vv) / norm_first
    proj_basis = scale * u_with - scale * shift * v_with - proj_second * cross
    on_u = on_u - proj_basis * scale
    on_v = on_v - proj_second / norm_first + proj_basis * scale * shift
    square_last = (
        on_z * (on_z * zz)
        + 2.0 * on_u * (on_z * uz)
        + 2.0 * on_v * (scale * vz)
        + on_u * (on_u * uu)
        + 2.0 * on_v * (on_u * vu)
        + on_v * (on_v * vv)
    )
    norm_last = jnp.sqrt(square_last + epsilon)
    for l in range(leaves):
        rows = pl.ds(l * nrhs, nrhs)
        v = vector[l]
        u = image[rows, :]
        basis_ref[l] = scale * u - (scale * shift) * v
        remainder_ref[l] = scale * second[rows, :] + on_u * u + on_v * v
    entries = (proj_first, norm_image, proj_second, proj_basis, norm_last)
    row, col = row_col((nrhs, nrhs))
    for i, entry in enumerate(entries):
        line = jnp.sum(jnp.where(row == col, entry, 0.0), axis=0, keepdims=True)
        hessenberg_ref[i : i + 1] = line


def shards(
    vector,
    near_cols,
    near_blocks,
    col_basis,
    row_basis,
    leaf_far,
    leaf_coupling,
    leaf_transfer,
    box_far,
    box_coupling,
    box_transfer,
    coarse_far,
    coarse_coupling,
):
    leaves, nrhs, width = vector.shape
    group = lax.axis_size(GRP)
    rows = lax.axis_size(ROWS)
    devices = rows * group
    kn = near_cols.shape[1]
    lanes = leaves * R
    flat = leaves * nrhs
    dense = nrhs * R // lanes
    tiles = width // lanes
    side = (leaves * tiles + 2 * group) * nrhs
    params = pltpu.CompilerParams(vmem_limit_bytes=LIMIT)

    given = {id(a) for a in (
        vector, near_cols, near_blocks, col_basis, row_basis, leaf_far, leaf_coupling,
        leaf_transfer, box_far, box_coupling, box_transfer, coarse_far, coarse_coupling,
    )}

    def placed(arrays):
        return [
            pltpu.with_memory_space_constraint(a, pltpu.HBM if id(a) in given else pltpu.VMEM)
            for a in arrays
        ]

    def made(*dims, dtype=F32):
        return pltpu.VMEM(dims, dtype)

    def call(kernel, inputs, outs, smem=(), hbm=(), scratch=()):
        specs = [SMEM] * len(smem) + [VMEM] * len(inputs)
        specs += [pl.BlockSpec(memory_space=pl.ANY)] * len(hbm)
        return pl.pallas_call(
            kernel,
            in_specs=specs,
            out_specs=[VMEM] * len(outs),
            out_shape=outs,
            scratch_shapes=scratch,
            compiler_params=params,
        )(*placed(smem), *placed(inputs), *placed(hbm))

    half = group // 2
    across = []
    for i in range(rows - 1):
        for j in range(half):
            pair = (i * group + group - 1 - j, (i + 1) * group + j)
            across += [pair, pair[::-1]]

    def swap(array, bits):
        return lax.ppermute(array, ROWS_GRP, [(i, i ^ bits) for i in range(devices)])

    def exchange(field, coef, number):
        mine, parent = call(
            group_kernel,
            [field, coef, swap(coef, 1), swap(coef, 3), swap(coef, 2)],
            [made(side, lanes, dtype=BF), made(rows, dense, lanes, dtype=BF)],
        )
        near_side = lax.ppermute(mine, ROWS_GRP, across)
        parents = lax.all_to_all(parent, ROWS, 0, 0, tiled=True)
        far_side = swap(near_side, half)
        chip = swap(field, 1)
        cross = swap(field, 3)
        (near,) = call(
            near_kernel,
            [field, chip, cross, near_side],
            [made(flat, width)],
            smem=[near_cols],
            hbm=[near_blocks],
            scratch=[
                pltpu.VMEM((group + 2, leaves * tiles * nrhs, lanes), BF),
                pltpu.VMEM((leaves, kn, width, width), BF),
                pltpu.SemaphoreType.DMA((leaves,)),
            ],
        )
        inputs = [mine, near_side, far_side, leaf_coupling, box_coupling, leaf_transfer]
        outs = [made(flat, lanes)]
        kernel = fine_kernel
        if number == 0:
            kernel = fine_and_stage_kernel
            inputs += [coarse_coupling, box_transfer, row_basis, col_basis, vector]
            outs += [
                made(R, lanes, dtype=BF), made(lanes, R, dtype=BF),
                made(lanes, width, dtype=BF), made(lanes, width, dtype=BF),
                made(lanes, R, dtype=BF), made(R, R, dtype=BF), made(*vector.shape),
            ]
        local_field, *staged = call(
            kernel,
            inputs,
            outs,
            smem=[leaf_far, box_far],
            scratch=[pltpu.VMEM((3 * group, 2 * nrhs, lanes), BF)],
        )
        return [parents, near, local_field], staged

    upward_out = [
        made(leaves * tiles * nrhs, lanes, dtype=BF), made(2 * nrhs, lanes, dtype=BF),
    ]
    stack = pltpu.VMEM((coarse_far.shape[1] * dense, lanes), F32)
    upward = call(start_kernel, [vector, col_basis, leaf_transfer, box_transfer], upward_out)
    received, staged = exchange(*upward, 0)
    coarse, down, row_flat, col_flat, leaf_up, box_up, first = staged
    image, *upward = call(
        middle_kernel,
        received + [coarse, down, row_flat, col_flat, leaf_up, box_up],
        [made(flat, width), *upward_out],
        smem=[coarse_far],
        scratch=[stack],
    )
    received, _ = exchange(*upward, 1)
    second, sums = call(
        products_kernel,
        received + [coarse, down, row_flat, first, image],
        [made(flat, width), made(devices, 1, 8 * nrhs)],
        smem=[coarse_far],
        scratch=[stack],
    )
    sums = lax.all_to_all(sums, ROWS_GRP, 0, 0, tiled=True)
    shape = jax.ShapeDtypeStruct
    basis, remainder, hessenberg = call(
        finish_kernel,
        [sums, first, image, second],
        [shape(vector.shape, F32), shape(vector.shape, F32), shape((5, nrhs), F32)],
    )
    return basis, remainder, hessenberg.T


def solution(mesh):
    finer = Mesh(
        mesh.devices.reshape(4, 4, 4, 2, 2), ("rows_0", "rows_1", "rows_2", "grp_0", "grp_1")
    )
    placed = (
        P(ROWS_GRP, None, None),
        P(ROWS_GRP, None),
        P(ROWS_GRP, None, None, None),
        P(ROWS_GRP, None, None),
        P(ROWS_GRP, None, None),
        P(ROWS_GRP, None),
        P(ROWS_GRP, None, None),
        P(ROWS_GRP, None, None),
        P(ROWS_GRP, None),
        P(ROWS_GRP, None, None),
        P(ROWS_GRP, None, None),
        P(ROWS, None),
        P(ROWS, None, None),
    )
    return jax.shard_map(
        shards,
        mesh=finer,
        in_specs=placed,
        out_specs=(P(ROWS_GRP, None, None), P(ROWS_GRP, None, None), P()),
        check_vma=False,
    )
```

```python
import jax
import jax.numpy as jnp
from jax import lax
from jax.experimental import pallas as pl
from jax.experimental.pallas import tpu as pltpu
from jax.sharding import Mesh
from jax.sharding import PartitionSpec as P


R = 32
GRP = ("grp_0", "grp_1")
ROWS = ("rows_0", "rows_1", "rows_2")
ROWS_GRP = ("rows_0", "rows_1", "rows_2", "grp_0", "grp_1")
BF = jnp.bfloat16
F32 = jnp.float32

epsilon = 1e-06
SMALL = 2.0**-40
SWITCH = 2.0**-20
LIMIT = 16 * 2**20

NT = (((1,), (1,)), ((), ()))
NN = (((1,), (0,)), ((), ()))

VMEM = pl.BlockSpec(memory_space=pltpu.VMEM)
SMEM = pl.BlockSpec(memory_space=pltpu.SMEM)


def dot(left, right, dims=NN):
    return lax.dot_general(left, right, dims, preferred_element_type=F32)


def row_col(shape):
    return (
        lax.broadcasted_iota(jnp.int32, shape, 0),
        lax.broadcasted_iota(jnp.int32, shape, 1),
    )


def diagonal(leaves, nrhs):
    row, col = row_col((leaves * nrhs, leaves * R))
    return row // nrhs == col // R


def over_leaves(array, leaves):
    step = array.shape[0] // leaves
    total = array[:step]
    for l in range(1, leaves):
        total = total + array[l * step : (l + 1) * step]
    return total


def transfers(leaf_transfer, box_transfer):
    lanes = leaf_transfer.shape[0]
    row, col = row_col((R, lanes))
    spread = (row == col % R).astype(BF)
    tiled = dot(leaf_transfer.astype(BF), spread).astype(BF)
    wide = dot(box_transfer.astype(BF), spread)
    wide = jnp.concatenate([wide] * (lanes // R), axis=0)
    row, col = row_col((lanes, lanes))
    return tiled, jnp.where(row // R == col // R, wide, 0.0).astype(BF)


def coefficients(field_bf, col_basis, leaf_transfer, box_transfer, packet_ref, coef_ref):
    lanes = col_basis.shape[0]
    leaves = lanes // R
    nrhs = field_bf.shape[0] // leaves
    full = dot(field_bf, col_basis, NT)
    leaf = over_leaves(jnp.where(diagonal(leaves, nrhs), full, 0.0), leaves).astype(BF)
    box = dot(leaf, leaf_transfer)
    row, col = row_col((nrhs, lanes))
    per_row = nrhs * R // lanes
    turned = jnp.where(row // per_row == col // R, box, 0.0).astype(BF)
    box = jnp.where(col < R, box, 0.0).astype(BF)
    row, col = row_col((nrhs, nrhs))
    picked = dot(((row == col % per_row) & (row < per_row)).astype(BF), turned).astype(BF)
    parent = dot(picked, box_transfer).astype(BF)
    blocks = []
    for l in range(leaves):
        for t in range(field_bf.shape[1] // lanes):
            blocks.append(field_bf[l * nrhs : (l + 1) * nrhs, t * lanes : (t + 1) * lanes])
    coef = [leaf, box, parent]
    packet_ref[...] = jnp.concatenate(blocks + coef, axis=0)
    coef_ref[...] = jnp.concatenate(coef, axis=0)


def start_kernel(vector, col_basis, leaf_transfer, box_transfer, packet_ref, coef_ref):
    leaves, nrhs, width = vector.shape
    field = vector[...].reshape(leaves * nrhs, width).astype(BF)
    up, across = transfers(leaf_transfer[...].reshape(leaves * R, R), box_transfer[0])
    coefficients(
        field, col_basis[...].reshape(leaves * R, width), up, across, packet_ref, coef_ref
    )


def group_kernel(own, chip, cross, coef, side_ref, parent_ref):
    size, _ = own.shape
    nrhs = coef.shape[0] // 3
    fields = size - 3 * nrhs
    per_row = parent_ref.shape[1]
    place = position()
    side_ref[:fields] = own[:fields]
    total = None
    for other, part in ((0, own[fields:]), (1, chip[fields:]), (3, cross[fields:]), (2, coef[...])):
        first = pl.multiple_of(fields + (place ^ other) * (2 * nrhs), 2 * nrhs)
        side_ref[pl.ds(first, 2 * nrhs)] = part[: 2 * nrhs]
        parent = part[2 * nrhs :].astype(F32)
        total = parent if total is None else total + parent
    dense = total.astype(BF)[:per_row]
    parent_ref[...] = jnp.broadcast_to(dense[None], parent_ref.shape)


def position():
    return lax.axis_index(GRP[0]) * lax.axis_size(GRP[1]) + lax.axis_index(GRP[1])


def row_index():
    index = lax.axis_index(ROWS[0])
    for axis in ROWS[1:]:
        index = index * lax.axis_size(axis) + lax.axis_index(axis)
    return index


def near_kernel(near_cols, own, chip, cross, side, blocks, out, window, weights, sems):
    leaves, kn, _, _ = blocks.shape
    nrhs = out.shape[0] // leaves
    group = window.shape[0] - 2
    fields = window.shape[1]
    copies = [
        pltpu.make_async_copy(blocks.at[l], weights.at[l], sems.at[l]) for l in range(leaves)
    ]
    for copy in copies:
        copy.start()
    window[0] = side[:fields]
    window[group + 1] = side[:fields]
    place = position()
    window[place + 1] = own[:fields]
    window[(place ^ 1) + 1] = chip[:fields]
    window[(place ^ 3) + 1] = cross[:fields]
    base = (row_index() * group - 1) * leaves
    tiles = fields // leaves // nrhs
    for l in range(leaves):
        picked = []
        for k in range(kn):
            index = near_cols[l, k] - base
            device = index // leaves
            first = (index - device * leaves) * (tiles * nrhs)
            picked += [
                window[device, pl.ds(pl.multiple_of(first + t * nrhs, nrhs), nrhs)]
                for t in range(tiles)
            ]
        copies[l].wait()
        total = None
        for k in range(kn):
            part = jnp.concatenate(picked[k * tiles : (k + 1) * tiles], axis=1)
            term = dot(part, weights[l, k], NT)
            total = term if total is None else total + term
        out[l * nrhs : (l + 1) * nrhs] = total


def fine_sums(
    leaf_far, box_far, own, side, other, leaf_coupling, box_coupling, leaf_transfer, out, window
):
    size, lanes = own.shape
    leaves, kf = leaf_far.shape
    nrhs = out.shape[0] // leaves
    group = window.shape[0] // 3
    fields = size - 2 * group * nrhs
    is_low = position() < group // 2
    side_slot = jnp.where(is_low, 0, 2 * group)
    other_slot = jnp.where(is_low, 2 * group, 0)
    for j in range(group):
        rows = slice(fields + j * 2 * nrhs, fields + (j + 1) * 2 * nrhs)
        window[side_slot + j] = side[rows]
        window[group + j] = own[rows]
        window[other_slot + j] = other[rows]
    first_box = (row_index() - 1) * group
    first_leaf = first_box * leaves
    _, col = row_col((nrhs, lanes))
    block = col // R
    per_tile = lanes // R
    rows = []
    for l in range(leaves):
        tiles = []
        for t in range(kf // per_tile):
            tile = jnp.zeros((nrhs, lanes), F32)
            for i in range(per_tile):
                index = leaf_far[l, t * per_tile + i] - first_leaf
                box = index // leaves
                item = index - box * leaves
                values = window[box, :nrhs].astype(F32)
                shift = lax.rem(i - item + per_tile, per_tile) * R
                values = pltpu.roll(values, shift, 1)
                tile = jnp.where(block == i, values, tile)
            tiles.append(tile.astype(BF))
        rows.append(jnp.concatenate(tiles, axis=1))
    gathered = jnp.concatenate(rows, axis=0)
    leaf_field = dot(gathered, leaf_coupling[...].reshape(leaves * R, -1), NT)
    tile = jnp.zeros((nrhs, lanes), F32)
    for k in range(box_far.shape[1]):
        values = window[box_far[0, k] - first_box, nrhs:].astype(F32)
        if k:
            values = pltpu.roll(values, k * R, 1)
        tile = jnp.where(block == k, values, tile)
    box_field = dot(tile.astype(BF), box_coupling[0], NT)
    transfer = leaf_transfer[...].reshape(leaves * R, R)
    shared = lax.dot_general(
        box_field, transfer, NT, precision=lax.Precision.HIGHEST, preferred_element_type=F32
    )
    out[...] = leaf_field + jnp.concatenate([shared] * leaves, axis=0)


def fine_kernel(
    leaf_far, box_far, own, side, other, leaf_coupling, box_coupling, leaf_transfer, out, window
):
    fine_sums(
        leaf_far, box_far, own, side, other, leaf_coupling, box_coupling, leaf_transfer, out,
        window,
    )


def fine_and_stage_kernel(
    leaf_far, box_far, own, side, other, leaf_coupling, box_coupling, leaf_transfer,
    coarse_coupling, box_transfer, row_basis, col_basis, vector, out, coarse_out, down_out,
    row_out, col_out, leaf_out, box_out, vector_out, window,
):
    fine_sums(
        leaf_far, box_far, own, side, other, leaf_coupling, box_coupling, leaf_transfer, out,
        window,
    )
    transfer = leaf_transfer[...].reshape(down_out.shape)
    coarse_out[...] = coarse_coupling[0]
    down_out[...] = lax.dot_general(
        transfer, box_transfer[0], NN, precision=lax.Precision.HIGHEST,
        preferred_element_type=F32,
    ).astype(BF)
    row_out[...] = row_basis[...].reshape(row_out.shape)
    col_out[...] = col_basis[...].reshape(col_out.shape)
    leaf_out[...], box_out[...] = transfers(transfer, box_transfer[0])
    vector_out[...] = vector[...]


def downward(coarse_far, parents, near, local_field, coarse_coupling, down, row_basis, stack):
    kc = coarse_far.shape[1]
    per_row, lanes = parents.shape[1:]
    leaves = lanes // R
    nrhs = near.shape[0] // leaves
    for k in range(kc):
        stack[k * per_row : (k + 1) * per_row] = parents[coarse_far[0, k]].astype(F32)
    dense = stack[...].astype(BF)
    row, col = row_col((kc * nrhs, kc * per_row))
    pick = (row // nrhs == col // per_row) & (row % per_row == col % per_row)
    wide = dot(pick.astype(BF), dense)
    row, col = row_col((kc * nrhs, lanes))
    wide = jnp.where(row % nrhs // per_row == col // R, wide, 0.0)
    half = wide + pltpu.roll(wide, 2 * R, 1)
    wide = half + pltpu.roll(half, R, 1)
    wide = jnp.where(row // nrhs == col // R, wide, 0.0)
    gathered = over_leaves(wide, kc).astype(BF)
    group_field = dot(gathered, coarse_coupling[...], NT)
    shared = dot(group_field.astype(BF), down[...], NT)
    local = local_field[...] + jnp.concatenate([shared] * leaves, axis=0)
    local = jnp.where(diagonal(leaves, nrhs), local, 0.0).astype(BF)
    return near[...] + dot(local, row_basis[...])


def middle_kernel(
    coarse_far, parents, near, local_field, coarse_coupling, down, row_basis, col_basis,
    leaf_transfer, box_transfer, image_ref, packet_ref, coef_ref, stack,
):
    image = downward(
        coarse_far, parents, near, local_field, coarse_coupling, down, row_basis, stack
    )
    image_ref[...] = image
    coefficients(
        image.astype(BF), col_basis[...], leaf_transfer[...], box_transfer[...], packet_ref,
        coef_ref,
    )


def products_kernel(
    coarse_far, parents, near, local_field, coarse_coupling, down, row_basis, vector, image,
    second_ref, sums_ref, stack,
):
    leaves, nrhs, width = vector.shape
    second = downward(
        coarse_far, parents, near, local_field, coarse_coupling, down, row_basis, stack
    )
    second_ref[...] = second
    first = vector[...].reshape(leaves * nrhs, width)
    middle = image[...]
    small = second * SMALL
    pairs = (
        (first, first), (first, middle), (middle, middle), (first, second),
        (middle, second), (second, second), (middle, small), (small, small),
    )
    parts = []
    for left, right in pairs:
        product = over_leaves(left * right, leaves)
        part = product[:, :128]
        for i in range(1, width // 128):
            part = part + product[:, i * 128 : (i + 1) * 128]
        parts.append(part)
    table = jnp.concatenate(parts, axis=0)
    sums = jnp.sum(table.T, axis=0, keepdims=True)
    sums_ref[...] = jnp.broadcast_to(sums[None], sums_ref.shape)


def finish_kernel(sums, vector, image, second, basis_ref, remainder_ref, hessenberg_ref):
    leaves, nrhs, width = vector.shape
    count = sums.shape[0] * leaves * width
    total = jnp.sum(sums[...], axis=0)
    row, col = row_col((nrhs, total.shape[1]))
    total = jnp.broadcast_to(total, (nrhs, total.shape[1]))

    def mean(i):
        own = jnp.where(col == i * nrhs + row, total, 0.0)
        return jnp.sum(own, axis=1, keepdims=True) / count

    vv, vu, uu, vz = mean(0), mean(1), mean(2), mean(3)
    large = mean(7) > SWITCH
    uz = jnp.where(large, mean(6), mean(4))
    zz = jnp.where(large, mean(7), mean(5))
    unit = jnp.where(large, 1.0 / SMALL, 1.0)
    square_first = vv + epsilon
    norm_first = jnp.sqrt(square_first)
    ratio = vu / square_first
    proj_first = 0.5 * vv / square_first + ratio
    shift = proj_first - 0.5
    square_image = (uu - 2.0 * shift * vu + shift * shift * vv) / square_first
    norm_image = jnp.sqrt(square_image + epsilon)
    scale = 1.0 / (norm_first * norm_image)
    on_z = scale * unit
    on_u = scale * (0.5 - shift)
    on_v = -0.5 * shift * scale
    v_with = scale * vz + on_u * vu + on_v * vv
    u_with = on_z * uz + on_u * uu + on_v * vu
    proj_second = v_with / norm_first
    cross = scale * (vu - shift * vv) / norm_first
    proj_basis = scale * u_with - scale * shift * v_with - proj_second * cross
    on_u = on_u - proj_basis * scale
    on_v = on_v - proj_second / norm_first + proj_basis * scale * shift
    square_last = (
        on_z * (on_z * zz)
        + 2.0 * on_u * (on_z * uz)
        + 2.0 * on_v * (scale * vz)
        + on_u * (on_u * uu)
        + 2.0 * on_v * (on_u * vu)
        + on_v * (on_v * vv)
    )
    norm_last = jnp.sqrt(square_last + epsilon)
    for l in range(leaves):
        rows = pl.ds(l * nrhs, nrhs)
        v = vector[l]
        u = image[rows, :]
        basis_ref[l] = scale * u - (scale * shift) * v
        remainder_ref[l] = scale * second[rows, :] + on_u * u + on_v * v
    entries = (proj_first, norm_image, proj_second, proj_basis, norm_last)
    row, col = row_col((nrhs, nrhs))
    for i, entry in enumerate(entries):
        line = jnp.sum(jnp.where(row == col, entry, 0.0), axis=0, keepdims=True)
        hessenberg_ref[i : i + 1] = line


def shards(
    vector,
    near_cols,
    near_blocks,
    col_basis,
    row_basis,
    leaf_far,
    leaf_coupling,
    leaf_transfer,
    box_far,
    box_coupling,
    box_transfer,
    coarse_far,
    coarse_coupling,
):
    leaves, nrhs, width = vector.shape
    group = lax.axis_size(GRP)
    rows = lax.axis_size(ROWS)
    devices = rows * group
    kn = near_cols.shape[1]
    lanes = leaves * R
    flat = leaves * nrhs
    dense = nrhs * R // lanes
    tiles = width // lanes
    size = (leaves * tiles + 3) * nrhs
    side = (leaves * tiles + 2 * group) * nrhs
    params = pltpu.CompilerParams(vmem_limit_bytes=LIMIT)

    given = {id(a) for a in (
        vector, near_cols, near_blocks, col_basis, row_basis, leaf_far, leaf_coupling,
        leaf_transfer, box_far, box_coupling, box_transfer, coarse_far, coarse_coupling,
    )}

    def placed(arrays):
        return [
            pltpu.with_memory_space_constraint(a, pltpu.HBM if id(a) in given else pltpu.VMEM)
            for a in arrays
        ]

    def made(*dims, dtype=F32):
        return pltpu.VMEM(dims, dtype)

    def call(kernel, inputs, outs, smem=(), hbm=(), scratch=()):
        specs = [SMEM] * len(smem) + [VMEM] * len(inputs)
        specs += [pl.BlockSpec(memory_space=pl.ANY)] * len(hbm)
        return pl.pallas_call(
            kernel,
            in_specs=specs,
            out_specs=[VMEM] * len(outs),
            out_shape=outs,
            scratch_shapes=scratch,
            compiler_params=params,
        )(*placed(smem), *placed(inputs), *placed(hbm))

    half = group // 2
    across = []
    for i in range(rows - 1):
        for j in range(half):
            pair = (i * group + group - 1 - j, (i + 1) * group + j)
            across += [pair, pair[::-1]]

    def swap(array, bits):
        return lax.ppermute(array, ROWS_GRP, [(i, i ^ bits) for i in range(devices)])

    def exchange(packet, coef, number):
        chip = swap(packet, 1)
        cross = swap(packet, 3)
        third = swap(coef, 2)
        mine, parent = call(
            group_kernel,
            [packet, chip, cross, third],
            [made(side, lanes, dtype=BF), made(rows, dense, lanes, dtype=BF)],
        )
        near_side = lax.ppermute(mine, ROWS_GRP, across)
        parents = lax.all_to_all(parent, ROWS, 0, 0, tiled=True)
        far_side = swap(near_side, half)
        (near,) = call(
            near_kernel,
            [packet, chip, cross, near_side],
            [made(flat, width)],
            smem=[near_cols],
            hbm=[near_blocks],
            scratch=[
                pltpu.VMEM((group + 2, leaves * tiles * nrhs, lanes), BF),
                pltpu.VMEM((leaves, kn, width, width), BF),
                pltpu.SemaphoreType.DMA((leaves,)),
            ],
        )
        inputs = [mine, near_side, far_side, leaf_coupling, box_coupling, leaf_transfer]
        outs = [made(flat, lanes)]
        kernel = fine_kernel
        if number == 0:
            kernel = fine_and_stage_kernel
            inputs += [coarse_coupling, box_transfer, row_basis, col_basis, vector]
            outs += [
                made(R, lanes, dtype=BF), made(lanes, R, dtype=BF),
                made(lanes, width, dtype=BF), made(lanes, width, dtype=BF),
                made(lanes, lanes, dtype=BF), made(lanes, lanes, dtype=BF), made(*vector.shape),
            ]
        local_field, *staged = call(
            kernel,
            inputs,
            outs,
            smem=[leaf_far, box_far],
            scratch=[pltpu.VMEM((3 * group, 2 * nrhs, lanes), BF)],
        )
        return [parents, near, local_field], staged

    upward_out = [made(size, lanes, dtype=BF), made(3 * nrhs, lanes, dtype=BF)]
    stack = pltpu.VMEM((coarse_far.shape[1] * dense, lanes), F32)
    upward = call(start_kernel, [vector, col_basis, leaf_transfer, box_transfer], upward_out)
    received, staged = exchange(*upward, 0)
    coarse, down, row_flat, col_flat, leaf_up, box_up, first = staged
    image, *upward = call(
        middle_kernel,
        received + [coarse, down, row_flat, col_flat, leaf_up, box_up],
        [made(flat, width), *upward_out],
        smem=[coarse_far],
        scratch=[stack],
    )
    received, _ = exchange(*upward, 1)
    second, sums = call(
        products_kernel,
        received + [coarse, down, row_flat, first, image],
        [made(flat, width), made(devices, 1, 8 * nrhs)],
        smem=[coarse_far],
        scratch=[stack],
    )
    sums = lax.all_to_all(sums, ROWS_GRP, 0, 0, tiled=True)
    shape = jax.ShapeDtypeStruct
    basis, remainder, hessenberg = call(
        finish_kernel,
        [sums, first, image, second],
        [shape(vector.shape, F32), shape(vector.shape, F32), shape((5, nrhs), F32)],
    )
    return basis, remainder, hessenberg.T


def solution(mesh):
    finer = Mesh(
        mesh.devices.reshape(4, 4, 4, 2, 2), ("rows_0", "rows_1", "rows_2", "grp_0", "grp_1")
    )
    placed = (
        P(ROWS_GRP, None, None),
        P(ROWS_GRP, None),
        P(ROWS_GRP, None, None, None),
        P(ROWS_GRP, None, None),
        P(ROWS_GRP, None, None),
        P(ROWS_GRP, None),
        P(ROWS_GRP, None, None),
        P(ROWS_GRP, None, None),
        P(ROWS_GRP, None),
        P(ROWS_GRP, None, None),
        P(ROWS_GRP, None, None),
        P(ROWS, None),
        P(ROWS, None, None),
    )
    return jax.shard_map(
        shards,
        mesh=finer,
        in_specs=placed,
        out_specs=(P(ROWS_GRP, None, None), P(ROWS_GRP, None, None), P()),
        check_vma=False,
    )
```

```python
import jax
import jax.numpy as jnp
from jax import lax
from jax.experimental import pallas as pl
from jax.experimental.pallas import tpu as pltpu
from jax.sharding import Mesh
from jax.sharding import PartitionSpec as P


R = 32
GRP = ("grp_0", "grp_1")
ROWS = ("rows_0", "rows_1", "rows_2")
ROWS_GRP = ("rows_0", "rows_1", "rows_2", "grp_0", "grp_1")
BF = jnp.bfloat16
F32 = jnp.float32

epsilon = 1e-06
SMALL = 2.0**-40
SWITCH = 2.0**-20
LIMIT = 16 * 2**20

NT = (((1,), (1,)), ((), ()))
NN = (((1,), (0,)), ((), ()))

VMEM = pl.BlockSpec(memory_space=pltpu.VMEM)
SMEM = pl.BlockSpec(memory_space=pltpu.SMEM)


def dot(left, right, dims=NN):
    return lax.dot_general(left, right, dims, preferred_element_type=F32)


def row_col(shape):
    return (
        lax.broadcasted_iota(jnp.int32, shape, 0),
        lax.broadcasted_iota(jnp.int32, shape, 1),
    )


def diagonal(leaves, nrhs):
    row, col = row_col((leaves * nrhs, leaves * R))
    return row // nrhs == col // R


def over_leaves(array, leaves):
    step = array.shape[0] // leaves
    total = array[:step]
    for l in range(1, leaves):
        total = total + array[l * step : (l + 1) * step]
    return total


def transfers(leaf_transfer, box_transfer):
    lanes = leaf_transfer.shape[0]
    row, col = row_col((R, lanes))
    spread = (row == col % R).astype(BF)
    tiled = dot(leaf_transfer.astype(BF), spread).astype(BF)
    wide = dot(box_transfer.astype(BF), spread)
    wide = jnp.concatenate([wide] * (lanes // R), axis=0)
    row, col = row_col((lanes, lanes))
    return tiled, jnp.where(row // R == col // R, wide, 0.0).astype(BF)


def coefficients(field_bf, col_basis, leaf_transfer, box_transfer, packet_ref, coef_ref):
    lanes = col_basis.shape[0]
    leaves = lanes // R
    nrhs = field_bf.shape[0] // leaves
    full = dot(field_bf, col_basis, NT)
    leaf = over_leaves(jnp.where(diagonal(leaves, nrhs), full, 0.0), leaves).astype(BF)
    box = dot(leaf, leaf_transfer)
    row, col = row_col((nrhs, lanes))
    per_row = nrhs * R // lanes
    turned = jnp.where(row // per_row == col // R, box, 0.0).astype(BF)
    box = jnp.where(col < R, box, 0.0).astype(BF)
    row, col = row_col((nrhs, nrhs))
    picked = dot(((row == col % per_row) & (row < per_row)).astype(BF), turned).astype(BF)
    parent = dot(picked, box_transfer).astype(BF)
    blocks = []
    for l in range(leaves):
        for t in range(field_bf.shape[1] // lanes):
            blocks.append(field_bf[l * nrhs : (l + 1) * nrhs, t * lanes : (t + 1) * lanes])
    coef = [leaf, box, parent]
    packet_ref[...] = jnp.concatenate(blocks + coef, axis=0)
    coef_ref[...] = jnp.concatenate(coef, axis=0)


def start_kernel(vector, col_basis, leaf_transfer, box_transfer, packet_ref, coef_ref):
    leaves, nrhs, width = vector.shape
    field = vector[...].reshape(leaves * nrhs, width).astype(BF)
    up, across = transfers(leaf_transfer[...].reshape(leaves * R, R), box_transfer[0])
    coefficients(
        field, col_basis[...].reshape(leaves * R, width), up, across, packet_ref, coef_ref
    )


def group_kernel(own, chip, cross, coef, side_ref, parent_ref):
    size, _ = own.shape
    nrhs = coef.shape[0] // 3
    fields = size - 3 * nrhs
    per_row = parent_ref.shape[1]
    place = position()
    side_ref[:fields] = own[:fields]
    total = None
    for other, part in ((0, own[fields:]), (1, chip[fields:]), (3, cross[fields:]), (2, coef[...])):
        first = pl.multiple_of(fields + (place ^ other) * (2 * nrhs), 2 * nrhs)
        side_ref[pl.ds(first, 2 * nrhs)] = part[: 2 * nrhs]
        parent = part[2 * nrhs :].astype(F32)
        total = parent if total is None else total + parent
    dense = total.astype(BF)[:per_row]
    parent_ref[...] = jnp.broadcast_to(dense[None], parent_ref.shape)


def position():
    return lax.axis_index(GRP[0]) * lax.axis_size(GRP[1]) + lax.axis_index(GRP[1])


def row_index():
    index = lax.axis_index(ROWS[0])
    for axis in ROWS[1:]:
        index = index * lax.axis_size(axis) + lax.axis_index(axis)
    return index


def near_kernel(near_cols, own, chip, cross, side, blocks, out, window, weights, sems):
    leaves, kn, _, _ = blocks.shape
    nrhs = out.shape[0] // leaves
    group = window.shape[0] - 2
    fields = window.shape[1]
    copies = [
        pltpu.make_async_copy(blocks.at[l], weights.at[l], sems.at[l]) for l in range(leaves)
    ]
    for copy in copies:
        copy.start()
    window[0] = side[:fields]
    window[group + 1] = side[:fields]
    place = position()
    window[place + 1] = own[:fields]
    window[(place ^ 1) + 1] = chip[:fields]
    window[(place ^ 3) + 1] = cross[:fields]
    base = (row_index() * group - 1) * leaves
    tiles = fields // leaves // nrhs
    for l in range(leaves):
        picked = []
        for k in range(kn):
            index = near_cols[l, k] - base
            device = index // leaves
            first = (index - device * leaves) * (tiles * nrhs)
            picked += [
                window[device, pl.ds(pl.multiple_of(first + t * nrhs, nrhs), nrhs)]
                for t in range(tiles)
            ]
        copies[l].wait()
        joined = jnp.concatenate([weights[l, k] for k in range(kn)], axis=1)
        total = dot(jnp.concatenate(picked, axis=1), joined, NT)
        out[l * nrhs : (l + 1) * nrhs] = total


def fine_sums(
    leaf_far, box_far, own, side, other, leaf_coupling, box_coupling, leaf_transfer, out, window
):
    size, lanes = own.shape
    leaves, kf = leaf_far.shape
    nrhs = out.shape[0] // leaves
    group = window.shape[0] // 3
    fields = size - 2 * group * nrhs
    is_low = position() < group // 2
    side_slot = jnp.where(is_low, 0, 2 * group)
    other_slot = jnp.where(is_low, 2 * group, 0)
    for j in range(group):
        rows = slice(fields + j * 2 * nrhs, fields + (j + 1) * 2 * nrhs)
        window[side_slot + j] = side[rows]
        window[group + j] = own[rows]
        window[other_slot + j] = other[rows]
    first_box = (row_index() - 1) * group
    first_leaf = first_box * leaves
    _, col = row_col((nrhs, lanes))
    block = col // R
    per_tile = lanes // R
    rows = []
    for l in range(leaves):
        tiles = []
        for t in range(kf // per_tile):
            tile = jnp.zeros((nrhs, lanes), F32)
            for i in range(per_tile):
                index = leaf_far[l, t * per_tile + i] - first_leaf
                box = index // leaves
                item = index - box * leaves
                values = window[box, :nrhs].astype(F32)
                shift = lax.rem(i - item + per_tile, per_tile) * R
                values = pltpu.roll(values, shift, 1)
                tile = jnp.where(block == i, values, tile)
            tiles.append(tile.astype(BF))
        rows.append(jnp.concatenate(tiles, axis=1))
    gathered = jnp.concatenate(rows, axis=0)
    leaf_field = dot(gathered, leaf_coupling[...].reshape(leaves * R, -1), NT)
    tile = jnp.zeros((nrhs, lanes), F32)
    for k in range(box_far.shape[1]):
        values = window[box_far[0, k] - first_box, nrhs:].astype(F32)
        if k:
            values = pltpu.roll(values, k * R, 1)
        tile = jnp.where(block == k, values, tile)
    box_field = dot(tile.astype(BF), box_coupling[0], NT)
    transfer = leaf_transfer[...].reshape(leaves * R, R)
    shared = lax.dot_general(
        box_field, transfer, NT, precision=lax.Precision.HIGHEST, preferred_element_type=F32
    )
    out[...] = leaf_field + jnp.concatenate([shared] * leaves, axis=0)


def fine_kernel(
    leaf_far, box_far, own, side, other, leaf_coupling, box_coupling, leaf_transfer, out, window
):
    fine_sums(
        leaf_far, box_far, own, side, other, leaf_coupling, box_coupling, leaf_transfer, out,
        window,
    )


def fine_and_stage_kernel(
    leaf_far, box_far, own, side, other, leaf_coupling, box_coupling, leaf_transfer,
    coarse_coupling, box_transfer, row_basis, col_basis, vector, out, coarse_out, down_out,
    row_out, col_out, leaf_out, box_out, vector_out, window,
):
    fine_sums(
        leaf_far, box_far, own, side, other, leaf_coupling, box_coupling, leaf_transfer, out,
        window,
    )
    transfer = leaf_transfer[...].reshape(down_out.shape)
    coarse_out[...] = coarse_coupling[0]
    down_out[...] = lax.dot_general(
        transfer, box_transfer[0], NN, precision=lax.Precision.HIGHEST,
        preferred_element_type=F32,
    ).astype(BF)
    row_out[...] = row_basis[...].reshape(row_out.shape)
    col_out[...] = col_basis[...].reshape(col_out.shape)
    leaf_out[...], box_out[...] = transfers(transfer, box_transfer[0])
    vector_out[...] = vector[...]


def downward(coarse_far, parents, near, local_field, coarse_coupling, down, row_basis, stack):
    kc = coarse_far.shape[1]
    per_row, lanes = parents.shape[1:]
    leaves = lanes // R
    nrhs = near.shape[0] // leaves
    for k in range(kc):
        stack[k * per_row : (k + 1) * per_row] = parents[coarse_far[0, k]].astype(F32)
    dense = stack[...].astype(BF)
    row, col = row_col((kc * nrhs, kc * per_row))
    pick = (row // nrhs == col // per_row) & (row % per_row == col % per_row)
    wide = dot(pick.astype(BF), dense)
    row, col = row_col((kc * nrhs, lanes))
    wide = jnp.where(row % nrhs // per_row == col // R, wide, 0.0)
    half = wide + pltpu.roll(wide, 2 * R, 1)
    wide = half + pltpu.roll(half, R, 1)
    wide = jnp.where(row // nrhs == col // R, wide, 0.0)
    gathered = over_leaves(wide, kc).astype(BF)
    group_field = dot(gathered, coarse_coupling[...], NT)
    shared = dot(group_field.astype(BF), down[...], NT)
    local = local_field[...] + jnp.concatenate([shared] * leaves, axis=0)
    local = jnp.where(diagonal(leaves, nrhs), local, 0.0).astype(BF)
    return near[...] + dot(local, row_basis[...])


def middle_kernel(
    coarse_far, parents, near, local_field, coarse_coupling, down, row_basis, col_basis,
    leaf_transfer, box_transfer, image_ref, packet_ref, coef_ref, stack,
):
    image = downward(
        coarse_far, parents, near, local_field, coarse_coupling, down, row_basis, stack
    )
    image_ref[...] = image
    coefficients(
        image.astype(BF), col_basis[...], leaf_transfer[...], box_transfer[...], packet_ref,
        coef_ref,
    )


def products_kernel(
    coarse_far, parents, near, local_field, coarse_coupling, down, row_basis, vector, image,
    second_ref, sums_ref, stack,
):
    leaves, nrhs, width = vector.shape
    second = downward(
        coarse_far, parents, near, local_field, coarse_coupling, down, row_basis, stack
    )
    second_ref[...] = second
    first = vector[...].reshape(leaves * nrhs, width)
    middle = image[...]
    small = second * SMALL
    pairs = (
        (first, first), (first, middle), (middle, middle), (first, second),
        (middle, second), (second, second), (middle, small), (small, small),
    )
    parts = []
    for left, right in pairs:
        product = over_leaves(left * right, leaves)
        part = product[:, :128]
        for i in range(1, width // 128):
            part = part + product[:, i * 128 : (i + 1) * 128]
        parts.append(part)
    table = jnp.concatenate(parts, axis=0)
    sums = jnp.sum(table.T, axis=0, keepdims=True)
    sums_ref[...] = jnp.broadcast_to(sums[None], sums_ref.shape)


def finish_kernel(sums, vector, image, second, basis_ref, remainder_ref, hessenberg_ref):
    leaves, nrhs, width = vector.shape
    count = sums.shape[0] * leaves * width
    total = jnp.sum(sums[...], axis=0)
    row, col = row_col((nrhs, total.shape[1]))
    total = jnp.broadcast_to(total, (nrhs, total.shape[1]))

    def mean(i):
        own = jnp.where(col == i * nrhs + row, total, 0.0)
        return jnp.sum(own, axis=1, keepdims=True) / count

    vv, vu, uu, vz = mean(0), mean(1), mean(2), mean(3)
    large = mean(7) > SWITCH
    uz = jnp.where(large, mean(6), mean(4))
    zz = jnp.where(large, mean(7), mean(5))
    unit = jnp.where(large, 1.0 / SMALL, 1.0)
    square_first = vv + epsilon
    norm_first = jnp.sqrt(square_first)
    ratio = vu / square_first
    proj_first = 0.5 * vv / square_first + ratio
    shift = proj_first - 0.5
    square_image = (uu - 2.0 * shift * vu + shift * shift * vv) / square_first
    norm_image = jnp.sqrt(jnp.maximum(square_image, 0.0) + epsilon)
    scale = 1.0 / (norm_first * norm_image)
    on_z = scale * unit
    on_u = scale * (0.5 - shift)
    on_v = -0.5 * shift * scale
    v_with = scale * vz + on_u * vu + on_v * vv
    u_with = on_z * uz + on_u * uu + on_v * vu
    proj_second = v_with / norm_first
    cross = scale * (vu - shift * vv) / norm_first
    proj_basis = scale * u_with - scale * shift * v_with - proj_second * cross
    on_u = on_u - proj_basis * scale
    on_v = on_v - proj_second / norm_first + proj_basis * scale * shift
    square_last = (
        on_z * (on_z * zz)
        + 2.0 * on_u * (on_z * uz)
        + 2.0 * on_v * (scale * vz)
        + on_u * (on_u * uu)
        + 2.0 * on_v * (on_u * vu)
        + on_v * (on_v * vv)
    )
    norm_last = jnp.sqrt(jnp.maximum(square_last, 0.0) + epsilon)
    for l in range(leaves):
        rows = pl.ds(l * nrhs, nrhs)
        v = vector[l]
        u = image[rows, :]
        basis_ref[l] = scale * u - (scale * shift) * v
        remainder_ref[l] = scale * second[rows, :] + on_u * u + on_v * v
    entries = (proj_first, norm_image, proj_second, proj_basis, norm_last)
    row, col = row_col((nrhs, nrhs))
    for i, entry in enumerate(entries):
        line = jnp.sum(jnp.where(row == col, entry, 0.0), axis=0, keepdims=True)
        hessenberg_ref[i : i + 1] = line


def shards(
    vector,
    near_cols,
    near_blocks,
    col_basis,
    row_basis,
    leaf_far,
    leaf_coupling,
    leaf_transfer,
    box_far,
    box_coupling,
    box_transfer,
    coarse_far,
    coarse_coupling,
):
    leaves, nrhs, width = vector.shape
    group = lax.axis_size(GRP)
    rows = lax.axis_size(ROWS)
    devices = rows * group
    kn = near_cols.shape[1]
    lanes = leaves * R
    flat = leaves * nrhs
    dense = nrhs * R // lanes
    tiles = width // lanes
    size = (leaves * tiles + 3) * nrhs
    side = (leaves * tiles + 2 * group) * nrhs
    params = pltpu.CompilerParams(vmem_limit_bytes=LIMIT)

    given = {id(a) for a in (
        vector, near_cols, near_blocks, col_basis, row_basis, leaf_far, leaf_coupling,
        leaf_transfer, box_far, box_coupling, box_transfer, coarse_far, coarse_coupling,
    )}

    def placed(arrays):
        return [
            pltpu.with_memory_space_constraint(a, pltpu.HBM if id(a) in given else pltpu.VMEM)
            for a in arrays
        ]

    def made(*dims, dtype=F32):
        return pltpu.VMEM(dims, dtype)

    def call(kernel, inputs, outs, smem=(), hbm=(), scratch=()):
        specs = [SMEM] * len(smem) + [VMEM] * len(inputs)
        specs += [pl.BlockSpec(memory_space=pl.ANY)] * len(hbm)
        return pl.pallas_call(
            kernel,
            in_specs=specs,
            out_specs=[VMEM] * len(outs),
            out_shape=outs,
            scratch_shapes=scratch,
            compiler_params=params,
        )(*placed(smem), *placed(inputs), *placed(hbm))

    half = group // 2
    across = []
    for i in range(rows - 1):
        for j in range(half):
            pair = (i * group + group - 1 - j, (i + 1) * group + j)
            across += [pair, pair[::-1]]

    def swap(array, bits):
        return lax.ppermute(array, ROWS_GRP, [(i, i ^ bits) for i in range(devices)])

    def exchange(packet, coef, number):
        chip = swap(packet, 1)
        cross = swap(packet, 3)
        third = swap(coef, 2)
        mine, parent = call(
            group_kernel,
            [packet, chip, cross, third],
            [made(side, lanes, dtype=BF), made(rows, dense, lanes, dtype=BF)],
        )
        near_side = lax.ppermute(mine, ROWS_GRP, across)
        parents = lax.all_to_all(parent, ROWS, 0, 0, tiled=True)
        far_side = swap(near_side, half)
        (near,) = call(
            near_kernel,
            [packet, chip, cross, near_side],
            [made(flat, width)],
            smem=[near_cols],
            hbm=[near_blocks],
            scratch=[
                pltpu.VMEM((group + 2, leaves * tiles * nrhs, lanes), BF),
                pltpu.VMEM((leaves, kn, width, width), BF),
                pltpu.SemaphoreType.DMA((leaves,)),
            ],
        )
        inputs = [mine, near_side, far_side, leaf_coupling, box_coupling, leaf_transfer]
        outs = [made(flat, lanes)]
        kernel = fine_kernel
        if number == 0:
            kernel = fine_and_stage_kernel
            inputs += [coarse_coupling, box_transfer, row_basis, col_basis, vector]
            outs += [
                made(R, lanes, dtype=BF), made(lanes, R, dtype=BF),
                made(lanes, width, dtype=BF), made(lanes, width, dtype=BF),
                made(lanes, lanes, dtype=BF), made(lanes, lanes, dtype=BF), made(*vector.shape),
            ]
        local_field, *staged = call(
            kernel,
            inputs,
            outs,
            smem=[leaf_far, box_far],
            scratch=[pltpu.VMEM((3 * group, 2 * nrhs, lanes), BF)],
        )
        return [parents, near, local_field], staged

    upward_out = [made(size, lanes, dtype=BF), made(3 * nrhs, lanes, dtype=BF)]
    stack = pltpu.VMEM((coarse_far.shape[1] * dense, lanes), F32)
    upward = call(start_kernel, [vector, col_basis, leaf_transfer, box_transfer], upward_out)
    received, staged = exchange(*upward, 0)
    coarse, down, row_flat, col_flat, leaf_up, box_up, first = staged
    image, *upward = call(
        middle_kernel,
        received + [coarse, down, row_flat, col_flat, leaf_up, box_up],
        [made(flat, width), *upward_out],
        smem=[coarse_far],
        scratch=[stack],
    )
    received, _ = exchange(*upward, 1)
    second, sums = call(
        products_kernel,
        received + [coarse, down, row_flat, first, image],
        [made(flat, width), made(devices, 1, 8 * nrhs)],
        smem=[coarse_far],
        scratch=[stack],
    )
    sums = lax.all_to_all(sums, ROWS_GRP, 0, 0, tiled=True)
    shape = jax.ShapeDtypeStruct
    basis, remainder, hessenberg = call(
        finish_kernel,
        [sums, first, image, second],
        [shape(vector.shape, F32), shape(vector.shape, F32), shape((5, nrhs), F32)],
    )
    return basis, remainder, hessenberg.T


def solution(mesh):
    finer = Mesh(
        mesh.devices.reshape(4, 4, 4, 2, 2), ("rows_0", "rows_1", "rows_2", "grp_0", "grp_1")
    )
    placed = (
        P(ROWS_GRP, None, None),
        P(ROWS_GRP, None),
        P(ROWS_GRP, None, None, None),
        P(ROWS_GRP, None, None),
        P(ROWS_GRP, None, None),
        P(ROWS_GRP, None),
        P(ROWS_GRP, None, None),
        P(ROWS_GRP, None, None),
        P(ROWS_GRP, None),
        P(ROWS_GRP, None, None),
        P(ROWS_GRP, None, None),
        P(ROWS, None),
        P(ROWS, None, None),
    )
    return jax.shard_map(
        shards,
        mesh=finer,
        in_specs=placed,
        out_specs=(P(ROWS_GRP, None, None), P(ROWS_GRP, None, None), P()),
        check_vma=False,
    )
```
